32 devices in a mesh: group: 4 (over y, core), dp: 2 (over x), mp: 4 (over z).
Axes of the slice: x: 2, y: 2, z: 4, core: 2. Of those that a mesh axis runs over, the one named last changes fastest.
Arguments:
- audio_states: bfloat16 [4, 1024, 1280], P('group', ('dp', 'mp')), may hold values from -6 to 6
- image_states: bfloat16 [4, 1024, 3200], P('group', ('dp', 'mp')), may hold values from -6 to 6
- audio_gain: float32 [1280], replicated, may hold values from 0.1 to 1.9
- image_gain: float32 [3200], replicated, may hold values from 0.1 to 1.9
- audio_proj: bfloat16 [1280, 8192], P('dp', 'mp'), may hold values from -1 to 1
- image_proj: bfloat16 [3200, 8192], P('dp', 'mp'), may hold values from -1 to 1
- block_rows: int32 [2, 2, 4], replicated, may hold values from 1 to 128
- destination: int32 [2, 2, 4], replicated, may hold values from 0 to 3, as said below
- input_gain: float32 [8192], P('mp'), may hold values from 0.1 to 1.9
- kv_weight: bfloat16 [8192, 2048], P('mp'), may hold values from -0.09375 to 0.09375
Outputs:
- key_values: bfloat16 [4, 1024, 2048], P('group', 'dp', 'mp')
- backbone_rows: bfloat16 [4, 1024, 8192], P('group', 'dp', 'mp')
The draws below stay inside these ranges and needn't reach their ends.
Inputs may be any that keep to these rules, and one draw needn't show every extreme that they name: `destination`: every backbone device receives exactly 2 blocks of each stream; an encoder index of dp sends either none or exactly 1 block of its stream to a backbone device.
All inputs are finite; a program needn't handle non-finite values.
Results may differ from the reference program's by a relative error of at most 0.012.
Values may be sent and summed in bfloat16 or wider, within the bound.
No kernel may reach another device: no remote copies, remote signals or barrier semaphores. Data moves between devices by JAX's collectives and lax.ppermute only.
A program may use at most 128 MiB of HBM per device.

```python
import jax
import jax.numpy as jnp
from jax import lax

AUDIO_WIDTH = 1280
IMAGE_WIDTH = 3200
MODEL_WIDTH = 8192
KV_WIDTH = 2048
BLOCK = 128
BLOCKS = 4
CAPACITY = 1
ROWS = 1024
N_DP = 2
N_MP = 4


def column_scaled(key, row_count, col_count):
    base_key, scale_key = jax.random.split(key)
    raw_values = jnp.clip(jax.random.normal(base_key, (row_count, col_count), jnp.float32), -5.0, 5.0)
    scales = jnp.exp(jax.random.uniform(scale_key, (col_count,), jnp.float32, 0.0, jnp.log(10.0)))
    return jnp.clip(raw_values * scales[None, :] / (4.0 * jnp.sqrt(row_count * 1.0)), -1.0, 1.0)


def draw_audio_proj(key, part):
    return column_scaled(jax.random.fold_in(key, 3), AUDIO_WIDTH, MODEL_WIDTH).astype(jnp.bfloat16)


def draw_image_proj(key, part):
    return column_scaled(jax.random.fold_in(key, 4), IMAGE_WIDTH, MODEL_WIDTH).astype(jnp.bfloat16)


def stream_routes(key):
    dest_count = 2 * N_DP
    groups_each = BLOCKS // CAPACITY
    half_count = groups_each // 2
    keys = jax.random.split(key, 5)
    spread_order = jax.random.permutation(keys[0], N_DP)
    even_offsets = jax.random.permutation(keys[1], N_DP)[:half_count] * 2
    odd_offsets = jax.random.permutation(keys[2], N_DP)[:half_count] * 2 + 1
    offsets = jax.random.permutation(keys[3], jnp.concatenate([even_offsets, odd_offsets]))
    targets = (2 * spread_order[:, None] + offsets[None, :]) % dest_count
    rotation = dest_count - targets[N_DP - 1, 0]
    targets = (targets + rotation) % dest_count
    block_keys = jax.random.split(keys[4], N_DP)
    orders = jax.vmap(lambda one_key: jax.random.permutation(one_key, BLOCKS))(block_keys)
    return jnp.take_along_axis(targets, orders // CAPACITY, axis=1).astype(jnp.int32)


def draw_destination(key, part):
    base_key = jax.random.fold_in(key, 7)
    return jnp.stack([stream_routes(jax.random.fold_in(base_key, 0)), stream_routes(jax.random.fold_in(base_key, 1))])


def place_ends(values, own_key, smallest, largest):
    longest = values.shape.index(max(values.shape))
    spots = []
    for shift in (0, 1):
        where = [jax.random.randint(jax.random.fold_in(own_key, axis), (), 0, length) for axis, length in enumerate(values.shape)]
        where[longest] = (where[longest] + shift) % values.shape[longest]
        spots.append(tuple(where))
    return values.at[spots[0]].set(smallest).at[spots[1]].set(largest)


def with_spikes(values, key, source, target, blocks, factor):
    owner, partner = [(jnp.arange(values.shape[dim]) // (values.shape[dim] // blocks)).reshape([-1 if axis == dim else 1 for axis in range(values.ndim)]) for dim in (source, target)]
    chosen = jax.random.permutation(key, blocks)[partner]
    strong = (owner == chosen) | (owner == (partner + blocks // 2) % blocks)
    return jnp.where(strong, factor * values, values)


def block_levels(own_key, shape, cuts, smallest, high):
    level, own = 1.0, jax.random.fold_in(own_key, 6)
    for dim, parts in cuts:
        heights = jnp.exp(jax.random.uniform(jax.random.fold_in(own, dim), (parts,), jnp.float32, smallest / len(cuts), high / len(cuts)))
        level = level * jnp.repeat(heights, shape[dim] // parts).reshape([-1 if axis == dim else 1 for axis in range(len(shape))])
    return level


def bell_draw(own_key, dims, scale, most, shards=(), kind=jnp.bfloat16):
    values = jax.random.normal(own_key, dims, jnp.float32) * scale
    if len(shards) > 0:
        values = block_levels(own_key, dims, shards, -0.22, 0.18) * values
    return jnp.clip(values, min=-most, max=most).astype(kind)


def gaussian_with(stream_key, extent, width, limit, shards, heavy, kind=jnp.bfloat16):
    array = width * jax.random.normal(stream_key, extent, jnp.float32)
    if shards:
        array = array * block_levels(stream_key, extent, shards, -0.22, 0.18)
    return jnp.clip(with_spikes(array, jax.random.fold_in(stream_key, 3), *heavy), -limit, limit).astype(kind)


def setup_inputs(seed: int = 0) -> dict:
    streams_of = jax.random.split(jax.random.key(seed), 11)
    return {
        "audio_states": bell_draw(streams_of[0], (4, ROWS, AUDIO_WIDTH), 1.0, 6.0, ((0, 4), (1, 8))),
        "image_states": bell_draw(streams_of[1], (4, ROWS, IMAGE_WIDTH), 1.0, 6.0, ((0, 4), (1, 8))),
        "audio_gain": jnp.clip(1.0 + 0.18 * jax.random.normal(streams_of[2], (AUDIO_WIDTH,), jnp.float32), 0.1, 1.9),
        "image_gain": jnp.clip(1.0 + 0.18 * jax.random.normal(streams_of[3], (IMAGE_WIDTH,), jnp.float32), 0.1, 1.9),
        "audio_proj": draw_audio_proj(jax.random.fold_in(streams_of[10], 71), 0),
        "image_proj": draw_image_proj(jax.random.fold_in(streams_of[10], 71), 0),
        "block_rows": place_ends(jax.random.randint(streams_of[6], (2, N_DP, BLOCKS), 1, BLOCK + 1), jax.random.fold_in(streams_of[6], 1), 1, BLOCK).astype(jnp.int32),
        "destination": draw_destination(jax.random.fold_in(streams_of[10], 71), 0),
        "input_gain": jnp.clip(1.0 + 0.18 * jax.random.normal(streams_of[8], (MODEL_WIDTH,), jnp.float32), 0.1, 1.9),
        "kv_weight": gaussian_with(streams_of[9], (MODEL_WIDTH, KV_WIDTH), MODEL_WIDTH ** -0.5, 0.09375, ((0, 4),), (0, 1, 4, 2.0)),
    }


EPS_LAYER = 1e-05
EPS_ROOT = 1e-06

def layer_norm(values_in, gain_vec):
    values = values_in.astype(jnp.float32)
    center = values - lax.optimization_barrier(jnp.mean(values, axis=-1, keepdims=True))
    spread = lax.optimization_barrier(jnp.mean(center * center, axis=-1, keepdims=True))
    return center * lax.rsqrt(spread + EPS_LAYER) * gain_vec

def to_blocks(states):
    width_in = states.shape[-1]
    split_rows = states.reshape(N_DP, N_MP, BLOCKS, BLOCK // N_MP, width_in)
    return split_rows.transpose(0, 2, 1, 3, 4).reshape(N_DP * BLOCKS, BLOCK, width_in)

def encode(states, gain_vec, limits, weight):
    width_in = states.shape[-1]
    normed = layer_norm(to_blocks(states), gain_vec)
    keep_rows = (jnp.arange(BLOCK, dtype=jnp.int32)[None, :] < limits.reshape(-1)[:, None]).astype(jnp.float32)
    normed = (normed * keep_rows[:, :, None]).astype(jnp.bfloat16)
    projected = jnp.dot(normed.reshape(-1, width_in), weight, preferred_element_type=jnp.float32).astype(jnp.bfloat16)
    return projected.reshape(N_DP * BLOCKS, BLOCK, MODEL_WIDTH)

def reference(audio_states, image_states, audio_gain, image_gain, audio_proj, image_proj, block_rows, destination, input_gain, kv_weight):
    audio_tokens = encode(audio_states[0], audio_gain, block_rows[0], audio_proj)
    image_tokens = encode(image_states[1], image_gain, block_rows[1], image_proj)
    every_block = jnp.concatenate([audio_tokens, image_tokens], axis=0)
    flat_dest = destination.reshape(-1).astype(jnp.int32)
    hit_table = (flat_dest[:, None] == jnp.arange(2 * N_DP, dtype=jnp.int32)[None, :]).astype(jnp.int32)
    dest_rank = lax.optimization_barrier(jnp.sum((jnp.cumsum(hit_table, axis=0) - 1) * hit_table, axis=1))
    placement = (flat_dest * BLOCKS + dest_rank).astype(jnp.int32)
    gathered = jnp.zeros_like(every_block).at[placement].set(every_block)
    tokens = gathered.reshape(-1, MODEL_WIDTH).astype(jnp.float32)
    mean_square = lax.optimization_barrier(jnp.mean(tokens * tokens, axis=1))
    scaled = (tokens * input_gain).astype(jnp.bfloat16)
    projected_heads = jnp.dot(scaled, kv_weight, preferred_element_type=jnp.float32)
    key_values = (projected_heads * lax.rsqrt(mean_square + EPS_ROOT)[:, None]).astype(jnp.bfloat16)
    key_values = key_values.reshape(2, N_DP * BLOCKS * BLOCK, KV_WIDTH)
    backbone_rows = gathered.reshape(2, N_DP * BLOCKS * BLOCK, MODEL_WIDTH)
    key_values_full = jnp.concatenate([jnp.zeros_like(key_values), key_values], axis=0)
    rows_full = jnp.concatenate([jnp.zeros_like(backbone_rows), backbone_rows], axis=0)
    return (key_values_full, rows_full)
```

```python
import functools

import jax
import jax.numpy as jnp
from jax import lax
from jax.experimental import pallas as pl
from jax.experimental.pallas import tpu as pltpu
from jax.sharding import PartitionSpec as P

BLOCK = 128
BLOCKS = 4


EPS_LAYER = 1e-05
EPS_ROOT = 1e-06


def layer_norm(values_in, gain_vec):
    values = values_in.astype(jnp.float32)
    center = values - jnp.mean(values, axis=-1, keepdims=True)
    spread = jnp.mean(center * center, axis=-1, keepdims=True)
    return center * lax.rsqrt(spread + EPS_LAYER) * gain_vec


def route_tables(destination, dest_count):
    flat_dest = destination.reshape(-1)
    hit_table = (flat_dest[:, None] == jnp.arange(dest_count, dtype=jnp.int32)[None, :]).astype(
        jnp.int32
    )
    dest_rank = jnp.sum((jnp.cumsum(hit_table, axis=0) - 1) * hit_table, axis=1)
    per_source = hit_table.reshape(-1, BLOCKS, dest_count)
    dest_slot = jnp.sum((jnp.cumsum(per_source, axis=1) - 1) * per_source, axis=2).reshape(-1)
    return (flat_dest, dest_rank, dest_slot)


def send_index(flat_dest, dest_slot, source, targets, capacity):
    row_dest = lax.dynamic_slice_in_dim(flat_dest, source * BLOCKS, BLOCKS)
    row_slot = lax.dynamic_slice_in_dim(dest_slot, source * BLOCKS, BLOCKS)
    wanted_slot = jnp.arange(capacity, dtype=jnp.int32)
    matches = (row_dest[None, None, :] == targets[:, None, None]) & (
        row_slot[None, None, :] == wanted_slot[None, :, None]
    )
    block_ids = jnp.arange(BLOCKS, dtype=jnp.int32)
    picked_index = jnp.sum(matches.astype(jnp.int32) * block_ids[None, None, :], axis=2).reshape(-1)
    present = jnp.any(matches, axis=2).reshape(-1)
    return (picked_index, present)


def route_blocks(blocks, streams, destination, group_id, dp_index):
    dp_count = lax.axis_size("dp")
    dest_count = 2 * dp_count
    capacity = BLOCKS // 4
    flat_dest, dest_rank, dest_slot = route_tables(destination, dest_count)
    serial = jnp.arange(dest_count, dtype=jnp.int32)
    outgoing = []
    for source_blocks, stream in zip(blocks, streams):
        picked_index, present = send_index(
            flat_dest, dest_slot, stream * dp_count + dp_index, serial, capacity
        )
        present = present & (group_id == stream)
        picked = jnp.take(source_blocks, picked_index, axis=0).reshape(dest_count * capacity, -1)
        outgoing.append(jnp.where(present[:, None], picked, jnp.zeros_like(picked)))
    packed = jnp.concatenate(outgoing, axis=1)
    spare_rows = jnp.zeros_like(packed)
    moved_rows = lax.all_to_all(
        jnp.concatenate([spare_rows, packed], axis=0),
        ("group", "dp"),
        split_axis=0,
        concat_axis=0,
        tiled=True,
    )
    arrived = moved_rows[: dest_count * capacity]
    my_index = (group_id - 2) * dp_count + dp_index
    on_backbone = group_id >= 2
    block_count = flat_dest.shape[0]
    source_slot = jnp.arange(block_count, dtype=jnp.int32) // BLOCKS * capacity + dest_slot
    results = []
    offset = 0
    for source_blocks, stream in zip(blocks, streams):
        slot_width = source_blocks[0].size
        columns = arrived[:, offset : offset + slot_width]
        offset = offset + slot_width
        wanted = stream * (BLOCKS // 2) + jnp.arange(BLOCKS // 2, dtype=jnp.int32)
        matches = (flat_dest[None, :] == my_index) & (dest_rank[None, :] == wanted[:, None])
        picked_index = jnp.sum(matches.astype(jnp.int32) * source_slot[None, :], axis=1)
        taken_rows = jnp.take(columns, picked_index, axis=0)
        taken_rows = jnp.where(on_backbone, taken_rows, jnp.zeros_like(taken_rows))
        results.append(taken_rows.reshape((wanted.shape[0],) + source_blocks.shape[1:]))
    return results


def project(audio_rows, image_rows, audio_active, image_active, audio_proj, image_proj):

    def folder(row_block, active, running, shard_part):
        return lax.cond(
            active,
            lambda inner: jnp.dot(row_block, shard_part, preferred_element_type=jnp.float32),
            lambda inner: inner,
            running,
        )

    audio_start = jnp.zeros((audio_rows.shape[0], audio_proj.shape[1]), jnp.float32)
    image_start = jnp.zeros((image_rows.shape[0], image_proj.shape[1]), jnp.float32)
    audio_out = folder(
        audio_rows, audio_active, audio_start, lax.all_gather(audio_proj, "dp", axis=0, tiled=True)
    )
    image_out = folder(
        image_rows, image_active, image_start, lax.all_gather(image_proj, "dp", axis=0, tiled=True)
    )
    return (audio_out, image_out)


def shards_general(
    audio_states,
    image_states,
    audio_gain,
    image_gain,
    audio_proj,
    image_proj,
    block_rows,
    destination,
    input_gain,
    kv_weight,
):
    group_id = lax.axis_index("group")
    dp_index = lax.axis_index("dp")
    mp_index = lax.axis_index("mp")
    mp_count = lax.axis_size("mp")
    share = BLOCK // mp_count
    row_ids = mp_index * share + jnp.arange(share, dtype=jnp.int32)

    def encode(states, gain_vec, stream):
        limits = lax.dynamic_index_in_dim(block_rows[stream], dp_index, 0, keepdims=False)
        keep_rows = (row_ids[None, :] < limits[:, None]).astype(jnp.float32)
        normed = layer_norm(states[0], gain_vec).reshape(BLOCKS, share, -1)
        return (normed * keep_rows[:, :, None]).astype(jnp.bfloat16)

    audio_normed = encode(audio_states, audio_gain, 0)
    image_normed = encode(image_states, image_gain, 1)
    on_backbone = group_id >= 2
    audio_part, image_part = route_blocks(
        (audio_normed, image_normed), (0, 1), destination, group_id, dp_index
    )
    audio_full, image_full = (
        lax.all_gather(audio_part, "mp", axis=1, tiled=True),
        lax.all_gather(image_part, "mp", axis=1, tiled=True),
    )
    audio_out, image_out = project(
        audio_full.reshape(-1, audio_full.shape[2]),
        image_full.reshape(-1, image_full.shape[2]),
        on_backbone,
        on_backbone,
        audio_proj,
        image_proj,
    )
    arrived = (
        jnp.concatenate([audio_out, image_out], axis=0)
        .astype(jnp.bfloat16)
        .reshape(BLOCKS, BLOCK, -1)
    )
    token_rows = arrived.reshape(BLOCKS * BLOCK, -1)
    tokens = token_rows.astype(jnp.float32)
    squares = lax.psum(jnp.sum(tokens * tokens, axis=1), "mp")
    scaled = (tokens * input_gain).astype(jnp.bfloat16)
    partial_value = jnp.dot(scaled, kv_weight, preferred_element_type=jnp.float32)
    summed = lax.psum_scatter(partial_value, "mp", scatter_dimension=1, tiled=True)
    full_width = tokens.shape[1] * mp_count
    result = summed * lax.rsqrt(squares / full_width + EPS_ROOT)[:, None]
    return (result.astype(jnp.bfloat16)[None], token_rows[None])


def smem():
    return pl.BlockSpec(memory_space=pltpu.SMEM)


def vmem():
    return pl.BlockSpec(memory_space=pltpu.VMEM)


def encode_kernel(stream, dp_count, meta, dest, limits, states, gain, *messages):
    group, dp, mp = meta[0], meta[1], meta[2]
    share = states.shape[0] // BLOCKS
    half = messages[0].shape[1]
    base = (stream * dp_count + dp) * BLOCKS

    @pl.when(group == stream)
    def _():
        for target in range(2 * dp_count):
            block = jnp.int32(0)
            for b in range(BLOCKS):
                block = jnp.where(dest[base + b] == target, b, block)
            limit = limits[base + block]
            start = pl.multiple_of(block * share, share)
            values = states[pl.ds(start, share), :].astype(jnp.float32)
            center = values - jnp.mean(values, axis=-1, keepdims=True)
            spread = jnp.mean(center * center, axis=-1, keepdims=True)
            normed = center * lax.rsqrt(spread + EPS_LAYER) * gain[...]
            row = mp * share + lax.broadcasted_iota(jnp.int32, normed.shape, 0)
            normed = jnp.where(row < limit, normed, 0.0).astype(jnp.bfloat16)
            c, home = target // dp_count, target % dp_count
            for k in range(dp_count):
                place = 0 if home == k else 1
                messages[c * dp_count + k][place * share : (place + 1) * share, :] = normed[
                    :, k * half : (k + 1) * half
                ]


def encode_stream(stream, dp_count, meta, dest, limits, states, gain):
    rows, width = states.shape
    shape = jax.ShapeDtypeStruct((2 * rows // BLOCKS, width // dp_count), jnp.bfloat16)
    return pl.pallas_call(
        functools.partial(encode_kernel, stream, dp_count),
        out_shape=[shape] * (2 * dp_count),
        in_specs=[smem(), smem(), smem(), vmem(), vmem()],
        out_specs=[vmem()] * (2 * dp_count),
        name="encode",
    )(meta, dest, limits, states, gain[None])


def project_kernel(mp_count, meta, *refs):
    pieces, weight, keep, send, rows = refs[:mp_count], *refs[mp_count:]
    share = pieces[0].shape[0] // 2
    block = share * mp_count

    @pl.when(pl.program_id(0) == 0)
    def _():
        for shift in range(mp_count):
            source = lax.rem(meta[2] + (mp_count - shift), mp_count)
            start = pl.multiple_of(source * share, share)
            rows[pl.ds(start, share), :] = pieces[shift][:share, :]
            rows[pl.ds(block + start, share), :] = pieces[shift][share:, :]

    out = jnp.dot(rows[...], weight[...], preferred_element_type=jnp.float32)
    keep[...] = out[:block]
    send[...] = out[block:].astype(jnp.bfloat16)


def project_rows(mp_count, meta, pieces, weight, tile):
    depth, width = weight.shape
    rows = pieces[0].shape[0] * mp_count
    return pl.pallas_call(
        functools.partial(project_kernel, mp_count),
        grid=(width // tile,),
        out_shape=[
            jax.ShapeDtypeStruct((rows // 2, width), jnp.float32),
            jax.ShapeDtypeStruct((rows // 2, width), jnp.bfloat16),
        ],
        in_specs=[smem()] + [vmem()] * mp_count + [pl.BlockSpec((depth, tile), lambda i: (0, i))],
        out_specs=[pl.BlockSpec((rows // 2, tile), lambda i: (0, i))] * 2,
        scratch_shapes=[pltpu.VMEM((rows, depth), jnp.bfloat16)],
        name="project",
    )(meta, *pieces, weight)


def heads_kernel(mp_count, meta, keep, other, gain, weight, tokens, squares, own, *rest):
    sends, scaled = rest[:-1], rest[-1]
    step = pl.program_id(0)

    @pl.when(step == 0)
    def _():
        rounded = (keep[...] + other[...].astype(jnp.float32)).astype(jnp.bfloat16)
        tokens[...] = rounded
        values = rounded.astype(jnp.float32)
        total = jnp.sum(values * values, axis=1, keepdims=True)
        turned = jnp.transpose(jnp.broadcast_to(total, (total.shape[0], 128)))
        squares[...] = turned[: squares.shape[0]]
        scaled[...] = (values * gain[...]).astype(jnp.bfloat16)

    out = jnp.dot(scaled[...], weight[...], preferred_element_type=jnp.float32)

    for shift in range(1, mp_count):

        @pl.when(step == shift - 1)
        def _():
            sends[shift - 1][...] = out.astype(jnp.bfloat16)

    @pl.when(step == mp_count - 1)
    def _():
        own[...] = out


def heads(mp_count, meta, keep, other, gain, weight):
    rows, width = keep.shape
    tile = weight.shape[1] // mp_count
    fixed = lambda i, meta: (0, 0)
    chunk = lambda i, meta: (0, lax.rem(meta[2] + i + 1, mp_count))
    return pl.pallas_call(
        functools.partial(heads_kernel, mp_count),
        grid_spec=pltpu.PrefetchScalarGridSpec(
            num_scalar_prefetch=1,
            grid=(mp_count,),
            in_specs=[
                pl.BlockSpec((rows, width), fixed),
                pl.BlockSpec((rows, width), fixed),
                pl.BlockSpec((1, width), fixed),
                pl.BlockSpec((width, tile), chunk),
            ],
            out_specs=[
                pl.BlockSpec((rows, width), fixed),
                pl.BlockSpec((8, rows), fixed),
                pl.BlockSpec((rows, tile), fixed),
            ]
            + [pl.BlockSpec((rows, tile), fixed)] * (mp_count - 1),
            scratch_shapes=[pltpu.VMEM((rows, width), jnp.bfloat16)],
        ),
        out_shape=[
            jax.ShapeDtypeStruct((rows, width), jnp.bfloat16),
            jax.ShapeDtypeStruct((8, rows), jnp.float32),
            jax.ShapeDtypeStruct((rows, tile), jnp.float32),
        ]
        + [jax.ShapeDtypeStruct((rows, tile), jnp.bfloat16)] * (mp_count - 1),
        name="heads",
    )(meta, keep, other, gain[None], weight)


def finish_kernel(full_width, own, own_squares, *refs):
    sums, squares, result = refs[: len(refs) // 2], refs[len(refs) // 2 : -1], refs[-1]
    total = own[...]
    for part in sums:
        total = total + part[...].astype(jnp.float32)
    square = own_squares[...]
    for part in squares:
        square = square + part[...]
    scale = lax.rsqrt(square[:1] / full_width + EPS_ROOT)
    column = jnp.transpose(jnp.broadcast_to(scale, (128, scale.shape[1])))[:, :1]
    result[...] = (total * column).astype(jnp.bfloat16)


def finish(full_width, own, own_squares, sums, squares):
    count = 2 + len(sums) + len(squares)
    return pl.pallas_call(
        functools.partial(finish_kernel, full_width),
        out_shape=jax.ShapeDtypeStruct(own.shape, jnp.bfloat16),
        in_specs=[vmem()] * count,
        out_specs=vmem(),
        name="finish",
    )(own, own_squares, *sums, *squares)


def shards_direct(
    audio_states,
    image_states,
    audio_gain,
    image_gain,
    audio_proj,
    image_proj,
    block_rows,
    destination,
    input_gain,
    kv_weight,
):
    group = lax.axis_index("group")
    dp = lax.axis_index("dp")
    mp = lax.axis_index("mp")
    dp_count = lax.axis_size("dp")
    mp_count = lax.axis_size("mp")
    meta = jnp.stack([group, dp, mp]).astype(jnp.int32)
    dest = destination.reshape(-1)
    limits = block_rows.reshape(-1)
    rings = [[(i, (i + shift) % mp_count) for i in range(mp_count)] for shift in range(mp_count)]
    swap = [(i, (i + 1) % dp_count) for i in range(dp_count)]
    up = [(0, 2), (1, 3)]
    on_backbone = group >= 2
    mine = lax.rem(group, 2) * dp_count + dp
    full_width = input_gain.shape[0] * mp_count

    streams = (
        (audio_states, audio_gain, audio_proj),
        (image_states, image_gain, image_proj),
    )
    gathered = []
    for stream, (states, gain, _) in enumerate(streams):
        messages = encode_stream(stream, dp_count, meta, dest, limits, states[0], gain)
        piece = None
        for c in range(2):
            for k in range(dp_count):
                pairs = [
                    (stream * dp_count + d, (2 * d + c) * dp_count + k) for d in range(dp_count)
                ]
                index = c * dp_count + k
                moved = lax.ppermute(messages[index], ("group", "dp"), pairs)
                piece = moved if piece is None else jnp.where(mine == index, moved, piece)
        gathered.append(
            [piece] + [lax.ppermute(piece, "mp", rings[shift]) for shift in range(1, mp_count)]
        )
    partial = [
        project_rows(mp_count, meta, pieces, proj, 512)
        for pieces, (_, _, proj) in zip(gathered, streams)
    ]
    others = [lax.ppermute(send, "dp", swap) for _, send in partial]
    row_parts, head_parts = [], []
    for (keep, _), other in zip(partial, others):
        tokens, squares, own, *sends = heads(mp_count, meta, keep, other, input_gain, kv_weight)
        sums = [lax.ppermute(x, "mp", rings[shift]) for shift, x in enumerate(sends, 1)]
        parts = [lax.ppermute(squares, "mp", rings[shift]) for shift in range(1, mp_count)]
        values = finish(full_width, own, squares, sums, parts)
        row_parts += [lax.ppermute(tokens, "group", up), tokens]
        head_parts += [lax.ppermute(values, "group", up), values]
    rows_out = jnp.concatenate(row_parts, axis=0)
    heads_out = jnp.concatenate(head_parts, axis=0)
    rows_out = jnp.where(on_backbone, rows_out, jnp.zeros_like(rows_out))
    heads_out = jnp.where(on_backbone, heads_out, jnp.zeros_like(heads_out))
    return (heads_out[None], rows_out[None])


def solution(mesh):
    one_each = 2 * mesh.shape["dp"] == BLOCKS
    shards = shards_direct if one_each else shards_general
    in_specs = (
        P("group", ("dp", "mp"), None),
        P("group", ("dp", "mp"), None),
        P(),
        P(),
        P("dp", "mp"),
        P("dp", "mp"),
        P(),
        P(),
        P("mp"),
        P("mp", None),
    )
    out_specs = (P("group", "dp", "mp"), P("group", "dp", "mp"))
    return jax.shard_map(shards, mesh=mesh, in_specs=in_specs, out_specs=out_specs, check_vma=False)
```

```python
import functools

import jax
import jax.numpy as jnp
from jax import lax
from jax.experimental import pallas as pl
from jax.experimental.pallas import tpu as pltpu
from jax.sharding import PartitionSpec as P


BLOCK = 128
BLOCKS = 4


EPS_LAYER = 1e-05
EPS_ROOT = 1e-06


def layer_norm(values_in, gain_vec):
    values = values_in.astype(jnp.float32)
    center = values - jnp.mean(values, axis=-1, keepdims=True)
    spread = jnp.mean(center * center, axis=-1, keepdims=True)
    return center * lax.rsqrt(spread + EPS_LAYER) * gain_vec


def route_tables(destination, dest_count):
    flat_dest = destination.reshape(-1)
    hit_table = (flat_dest[:, None] == jnp.arange(dest_count, dtype=jnp.int32)[None, :]).astype(
        jnp.int32
    )
    dest_rank = jnp.sum((jnp.cumsum(hit_table, axis=0) - 1) * hit_table, axis=1)
    per_source = hit_table.reshape(-1, BLOCKS, dest_count)
    dest_slot = jnp.sum((jnp.cumsum(per_source, axis=1) - 1) * per_source, axis=2).reshape(-1)
    return (flat_dest, dest_rank, dest_slot)


def send_index(flat_dest, dest_slot, source, targets, capacity):
    row_dest = lax.dynamic_slice_in_dim(flat_dest, source * BLOCKS, BLOCKS)
    row_slot = lax.dynamic_slice_in_dim(dest_slot, source * BLOCKS, BLOCKS)
    wanted_slot = jnp.arange(capacity, dtype=jnp.int32)
    matches = (row_dest[None, None, :] == targets[:, None, None]) & (
        row_slot[None, None, :] == wanted_slot[None, :, None]
    )
    block_ids = jnp.arange(BLOCKS, dtype=jnp.int32)
    picked_index = jnp.sum(matches.astype(jnp.int32) * block_ids[None, None, :], axis=2).reshape(-1)
    present = jnp.any(matches, axis=2).reshape(-1)
    return (picked_index, present)


def route_blocks(blocks, streams, destination, group_id, dp_index):
    dp_count = lax.axis_size("dp")
    dest_count = 2 * dp_count
    capacity = BLOCKS // 4
    flat_dest, dest_rank, dest_slot = route_tables(destination, dest_count)
    serial = jnp.arange(dest_count, dtype=jnp.int32)
    outgoing = []
    for source_blocks, stream in zip(blocks, streams):
        picked_index, present = send_index(
            flat_dest, dest_slot, stream * dp_count + dp_index, serial, capacity
        )
        present = present & (group_id == stream)
        picked = jnp.take(source_blocks, picked_index, axis=0).reshape(dest_count * capacity, -1)
        outgoing.append(jnp.where(present[:, None], picked, jnp.zeros_like(picked)))
    packed = jnp.concatenate(outgoing, axis=1)
    spare_rows = jnp.zeros_like(packed)
    moved_rows = lax.all_to_all(
        jnp.concatenate([spare_rows, packed], axis=0),
        ("group", "dp"),
        split_axis=0,
        concat_axis=0,
        tiled=True,
    )
    arrived = moved_rows[: dest_count * capacity]
    my_index = (group_id - 2) * dp_count + dp_index
    on_backbone = group_id >= 2
    block_count = flat_dest.shape[0]
    source_slot = jnp.arange(block_count, dtype=jnp.int32) // BLOCKS * capacity + dest_slot
    results = []
    offset = 0
    for source_blocks, stream in zip(blocks, streams):
        slot_width = source_blocks[0].size
        columns = arrived[:, offset : offset + slot_width]
        offset = offset + slot_width
        wanted = stream * (BLOCKS // 2) + jnp.arange(BLOCKS // 2, dtype=jnp.int32)
        matches = (flat_dest[None, :] == my_index) & (dest_rank[None, :] == wanted[:, None])
        picked_index = jnp.sum(matches.astype(jnp.int32) * source_slot[None, :], axis=1)
        taken_rows = jnp.take(columns, picked_index, axis=0)
        taken_rows = jnp.where(on_backbone, taken_rows, jnp.zeros_like(taken_rows))
        results.append(taken_rows.reshape((wanted.shape[0],) + source_blocks.shape[1:]))
    return results


def project(audio_rows, image_rows, audio_active, image_active, audio_proj, image_proj):

    def folder(row_block, active, running, shard_part):
        return lax.cond(
            active,
            lambda inner: jnp.dot(row_block, shard_part, preferred_element_type=jnp.float32),
            lambda inner: inner,
            running,
        )

    audio_start = jnp.zeros((audio_rows.shape[0], audio_proj.shape[1]), jnp.float32)
    image_start = jnp.zeros((image_rows.shape[0], image_proj.shape[1]), jnp.float32)
    audio_out = folder(
        audio_rows, audio_active, audio_start, lax.all_gather(audio_proj, "dp", axis=0, tiled=True)
    )
    image_out = folder(
        image_rows, image_active, image_start, lax.all_gather(image_proj, "dp", axis=0, tiled=True)
    )
    return (audio_out, image_out)


def shards_general(
    audio_states,
    image_states,
    audio_gain,
    image_gain,
    audio_proj,
    image_proj,
    block_rows,
    destination,
    input_gain,
    kv_weight,
):
    group_id = lax.axis_index("group")
    dp_index = lax.axis_index("dp")
    mp_index = lax.axis_index("mp")
    mp_count = lax.axis_size("mp")
    share = BLOCK // mp_count
    row_ids = mp_index * share + jnp.arange(share, dtype=jnp.int32)

    def encode(states, gain_vec, stream):
        limits = lax.dynamic_index_in_dim(block_rows[stream], dp_index, 0, keepdims=False)
        keep_rows = (row_ids[None, :] < limits[:, None]).astype(jnp.float32)
        normed = layer_norm(states[0], gain_vec).reshape(BLOCKS, share, -1)
        return (normed * keep_rows[:, :, None]).astype(jnp.bfloat16)

    audio_normed = encode(audio_states, audio_gain, 0)
    image_normed = encode(image_states, image_gain, 1)
    on_backbone = group_id >= 2
    audio_part, image_part = route_blocks(
        (audio_normed, image_normed), (0, 1), destination, group_id, dp_index
    )
    audio_full, image_full = (
        lax.all_gather(audio_part, "mp", axis=1, tiled=True),
        lax.all_gather(image_part, "mp", axis=1, tiled=True),
    )
    audio_out, image_out = project(
        audio_full.reshape(-1, audio_full.shape[2]),
        image_full.reshape(-1, image_full.shape[2]),
        on_backbone,
        on_backbone,
        audio_proj,
        image_proj,
    )
    arrived = (
        jnp.concatenate([audio_out, image_out], axis=0)
        .astype(jnp.bfloat16)
        .reshape(BLOCKS, BLOCK, -1)
    )
    token_rows = arrived.reshape(BLOCKS * BLOCK, -1)
    tokens = token_rows.astype(jnp.float32)
    squares = lax.psum(jnp.sum(tokens * tokens, axis=1), "mp")
    scaled = (tokens * input_gain).astype(jnp.bfloat16)
    partial_value = jnp.dot(scaled, kv_weight, preferred_element_type=jnp.float32)
    summed = lax.psum_scatter(partial_value, "mp", scatter_dimension=1, tiled=True)
    full_width = tokens.shape[1] * mp_count
    result = summed * lax.rsqrt(squares / full_width + EPS_ROOT)[:, None]
    return (result.astype(jnp.bfloat16)[None], token_rows[None])


MIB = 1 << 20


def smem():
    return pl.BlockSpec(memory_space=pltpu.SMEM)


def vmem():
    return pl.BlockSpec(memory_space=pltpu.VMEM)


def limits_of(mib, flops=0):
    return dict(
        compiler_params=pltpu.CompilerParams(vmem_limit_bytes=mib * MIB),
        cost_estimate=pl.CostEstimate(flops=flops, transcendentals=0, bytes_accessed=0),
    )


def encode_kernel(dp_count, meta, dest, limits, *refs):
    group, dp, mp = meta[0], meta[1], meta[2]
    targets = 2 * dp_count
    inputs, messages = refs[:4], refs[4:]
    for stream in range(2):
        states, gain = inputs[2 * stream : 2 * stream + 2]
        outs = messages[stream * targets : (stream + 1) * targets]
        share = states.shape[1] // BLOCKS
        half = outs[0].shape[1]

        @pl.when(group == stream)
        def _():
            scale = gain[...].reshape(1, -1)
            for target in range(targets):
                block = jnp.int32(0)
                for b in range(BLOCKS):
                    block = jnp.where(dest[stream, dp, b] == target, b, block)
                limit = limits[stream, dp, block]
                start = pl.multiple_of(block * share, share)
                values = states[0, pl.ds(start, share), :].astype(jnp.float32)
                center = values - jnp.mean(values, axis=-1, keepdims=True)
                spread = jnp.mean(center * center, axis=-1, keepdims=True)
                normed = center * lax.rsqrt(spread + EPS_LAYER) * scale
                row = mp * share + lax.broadcasted_iota(jnp.int32, normed.shape, 0)
                normed = jnp.where(row < limit, normed, 0.0).astype(jnp.bfloat16)
                c, home = target // dp_count, target % dp_count
                for k in range(dp_count):
                    place = 0 if home == k else 1
                    outs[c * dp_count + k][place * share : (place + 1) * share, :] = normed[
                        :, k * half : (k + 1) * half
                    ]


def encode(dp_count, meta, dest, limits, streams):
    arguments, shapes = [], []
    for states, gain, _ in streams:
        _, rows, width = states.shape
        arguments += [states, gain]
        shape = jax.ShapeDtypeStruct((2 * rows // BLOCKS, width // dp_count), jnp.bfloat16)
        shapes += [shape] * (2 * dp_count)
    return pl.pallas_call(
        functools.partial(encode_kernel, dp_count),
        out_shape=shapes,
        in_specs=[smem()] * 3 + [vmem()] * len(arguments),
        out_specs=[vmem()] * len(shapes),
        name="encode",
        **limits_of(8, 1 << 28),
    )(meta, dest, limits, *arguments)


def project_kernel(mp_count, tile, meta, *refs):
    pieces, weight, keep, send, rows = refs[:mp_count], *refs[mp_count:]
    share = pieces[0].shape[0] // 2
    block = share * mp_count
    for shift in range(mp_count):
        source = lax.rem(meta[2] + (mp_count - shift), mp_count)
        start = pl.multiple_of(source * share, share)
        rows[pl.ds(start, share), :] = pieces[shift][:share, :]
        rows[pl.ds(block + start, share), :] = pieces[shift][share:, :]
    for first in range(0, weight.shape[1], tile):
        out = jnp.dot(
            rows[...], weight[:, first : first + tile], preferred_element_type=jnp.float32
        )
        keep[:, first : first + tile] = out[:block]
        send[:, first : first + tile] = out[block:].astype(jnp.bfloat16)


def project_rows(mp_count, meta, pieces, weight, tile):
    depth, width = weight.shape
    rows = pieces[0].shape[0] * mp_count
    return pl.pallas_call(
        functools.partial(project_kernel, mp_count, tile),
        out_shape=[
            jax.ShapeDtypeStruct((rows // 2, width), jnp.float32),
            jax.ShapeDtypeStruct((rows // 2, width), jnp.bfloat16),
        ],
        in_specs=[smem()] + [vmem()] * (mp_count + 1),
        out_specs=[vmem()] * 2,
        scratch_shapes=[pltpu.VMEM((rows, depth), jnp.bfloat16)],
        name="project",
        **limits_of(12, 2 * rows * depth * width),
    )(meta, *pieces, weight)


def heads_kernel(mp_count, meta, keep, other, gain, weight, tokens, own, *rest):
    sends, scaled = rest[:-1], rest[-1]
    rows, tile = own.shape[0] - 8, own.shape[1]
    rounded = (keep[...] + other[...].astype(jnp.float32)).astype(jnp.bfloat16)
    tokens[...] = rounded
    values = rounded.astype(jnp.float32)
    scaled[...] = (values * gain[...].reshape(1, -1)).astype(jnp.bfloat16)
    total = jnp.sum(values * values, axis=1, keepdims=True)
    turned = jnp.transpose(jnp.broadcast_to(total, (rows, 128)))[:8]
    high = turned.astype(jnp.bfloat16).astype(jnp.float32)
    line = lax.broadcasted_iota(jnp.int32, turned.shape, 0)
    packed = jnp.where(line == 0, high, jnp.where(line == 1, turned - high, 0.0))
    packed = jnp.concatenate([packed] + [jnp.zeros((8, tile - rows), jnp.float32)], axis=1)
    for shift in list(range(1, mp_count)) + [0]:
        chunk = lax.rem(meta[2] + shift, mp_count)
        columns = pl.ds(pl.multiple_of(chunk * tile, tile), tile)
        out = jnp.dot(scaled[...], weight[:, columns], preferred_element_type=jnp.float32)
        if shift:
            block = jnp.concatenate([out, packed], axis=0)
            sends[shift - 1][...] = block.astype(jnp.bfloat16)
        else:
            own[:rows, :] = out
            own[rows:, :] = packed


def heads(mp_count, meta, keep, other, gain, weight):
    rows, width = keep.shape
    tile = weight.shape[1] // mp_count
    return pl.pallas_call(
        functools.partial(heads_kernel, mp_count),
        in_specs=[smem()] + [vmem()] * 4,
        out_specs=[vmem()] * (1 + mp_count),
        scratch_shapes=[pltpu.VMEM((rows, width), jnp.bfloat16)],
        out_shape=[
            jax.ShapeDtypeStruct((rows, width), jnp.bfloat16),
            jax.ShapeDtypeStruct((rows + 8, tile), jnp.float32),
        ]
        + [jax.ShapeDtypeStruct((rows + 8, tile), jnp.bfloat16)] * (mp_count - 1),
        name="heads",
        **limits_of(14, 2 * rows * width * weight.shape[1]),
    )(meta, keep, other, gain, weight)


def finish_kernel(full_width, own, *refs):
    parts, result = refs[:-1], refs[-1]
    rows = result.shape[0]
    total = own[...]
    for part in parts:
        total = total + part[...].astype(jnp.float32)
    square = total[rows : rows + 1, :rows] + total[rows + 1 : rows + 2, :rows]
    scale = lax.rsqrt(square / full_width + EPS_ROOT)
    column = jnp.transpose(jnp.broadcast_to(scale, (128, rows)))[:, :1]
    result[...] = (total[:rows] * column).astype(jnp.bfloat16)


def finish(full_width, own, parts):
    rows, tile = own.shape
    return pl.pallas_call(
        functools.partial(finish_kernel, full_width),
        out_shape=jax.ShapeDtypeStruct((rows - 8, tile), jnp.bfloat16),
        in_specs=[vmem()] * (1 + len(parts)),
        out_specs=vmem(),
        name="finish",
        **limits_of(4, 1 << 26),
    )(own, *parts)


def shards_direct(
    audio_states,
    image_states,
    audio_gain,
    image_gain,
    audio_proj,
    image_proj,
    block_rows,
    destination,
    input_gain,
    kv_weight,
):
    group = lax.axis_index("group")
    dp = lax.axis_index("dp")
    mp = lax.axis_index("mp")
    dp_count = lax.axis_size("dp")
    mp_count = lax.axis_size("mp")
    meta = jnp.stack([group, dp, mp]).astype(jnp.int32)
    rings = [[(i, (i + shift) % mp_count) for i in range(mp_count)] for shift in range(mp_count)]
    swap = [(i, (i + 1) % dp_count) for i in range(dp_count)]
    up = [(0, 2), (1, 3)]
    on_backbone = group >= 2
    mine = lax.rem(group, 2) * dp_count + dp
    full_width = input_gain.shape[0] * mp_count
    targets = 2 * dp_count
    streams = (
        (audio_states, audio_gain, audio_proj),
        (image_states, image_gain, image_proj),
    )

    messages = encode(dp_count, meta, destination, block_rows, streams)
    gathered = []
    for stream in range(2):
        piece = None
        for index in range(targets):
            c, k = index // dp_count, index % dp_count
            pairs = [(stream * dp_count + d, (2 * d + c) * dp_count + k) for d in range(dp_count)]
            moved = lax.ppermute(messages[stream * targets + index], ("group", "dp"), pairs)
            piece = moved if piece is None else jnp.where(mine == index, moved, piece)
        pieces = [piece]
        for shift in range(1, mp_count):
            pieces.append(lax.ppermute(piece, "mp", rings[shift]))
        gathered.append(pieces)
    partial, others = [], []
    for stream, (_, _, proj) in enumerate(streams):
        partial.append(project_rows(mp_count, meta, gathered[stream], proj, 512))
        others.append(lax.ppermute(partial[stream][1], "dp", swap))
    row_parts, head_parts = [], []
    for stream in range(2):
        tokens, own, *sends = heads(
            mp_count, meta, partial[stream][0], others[stream], input_gain, kv_weight
        )
        sums = []
        for shift, part in enumerate(sends, 1):
            sums.append(lax.ppermute(part, "mp", rings[shift]))
        row_parts += [lax.ppermute(tokens, "group", up), tokens]
        values = finish(full_width, own, sums)
        head_parts += [lax.ppermute(values, "group", up), values]
    rows_out = jnp.concatenate(row_parts, axis=0)
    heads_out = jnp.concatenate(head_parts, axis=0)
    rows_out = jnp.where(on_backbone, rows_out, jnp.zeros_like(rows_out))
    heads_out = jnp.where(on_backbone, heads_out, jnp.zeros_like(heads_out))
    return (heads_out[None], rows_out[None])


def solution(mesh):
    if 2 * mesh.shape["dp"] != BLOCKS:
        return mapped(shards_general, mesh)
    layer = lambda *inputs: shards_direct(*inputs)
    return mapped(layer, mesh)


def mapped(shards, mesh):
    in_specs = (
        P("group", ("dp", "mp"), None),
        P("group", ("dp", "mp"), None),
        P(),
        P(),
        P("dp", "mp"),
        P("dp", "mp"),
        P(),
        P(),
        P("mp"),
        P("mp", None),
    )
    out_specs = (P("group", "dp", "mp"), P("group", "dp", "mp"))
    return jax.shard_map(shards, mesh=mesh, in_specs=in_specs, out_specs=out_specs, check_vma=False)
```

```python
import functools

import jax
import jax.numpy as jnp
from jax import lax
from jax.experimental import pallas as pl
from jax.experimental.pallas import tpu as pltpu
from jax.sharding import PartitionSpec as P


BLOCK = 128
BLOCKS = 4


EPS_LAYER = 1e-05
EPS_ROOT = 1e-06


def layer_norm(values_in, gain_vec):
    values = values_in.astype(jnp.float32)
    center = values - jnp.mean(values, axis=-1, keepdims=True)
    spread = jnp.mean(center * center, axis=-1, keepdims=True)
    return center * lax.rsqrt(spread + EPS_LAYER) * gain_vec


def route_tables(destination, dest_count):
    flat_dest = destination.reshape(-1)
    hit_table = (flat_dest[:, None] == jnp.arange(dest_count, dtype=jnp.int32)[None, :]).astype(
        jnp.int32
    )
    dest_rank = jnp.sum((jnp.cumsum(hit_table, axis=0) - 1) * hit_table, axis=1)
    per_source = hit_table.reshape(-1, BLOCKS, dest_count)
    dest_slot = jnp.sum((jnp.cumsum(per_source, axis=1) - 1) * per_source, axis=2).reshape(-1)
    return (flat_dest, dest_rank, dest_slot)


def send_index(flat_dest, dest_slot, source, targets, capacity):
    row_dest = lax.dynamic_slice_in_dim(flat_dest, source * BLOCKS, BLOCKS)
    row_slot = lax.dynamic_slice_in_dim(dest_slot, source * BLOCKS, BLOCKS)
    wanted_slot = jnp.arange(capacity, dtype=jnp.int32)
    matches = (row_dest[None, None, :] == targets[:, None, None]) & (
        row_slot[None, None, :] == wanted_slot[None, :, None]
    )
    block_ids = jnp.arange(BLOCKS, dtype=jnp.int32)
    picked_index = jnp.sum(matches.astype(jnp.int32) * block_ids[None, None, :], axis=2).reshape(-1)
    present = jnp.any(matches, axis=2).reshape(-1)
    return (picked_index, present)


def route_blocks(blocks, streams, destination, group_id, dp_index):
    dp_count = lax.axis_size("dp")
    dest_count = 2 * dp_count
    capacity = BLOCKS // 4
    flat_dest, dest_rank, dest_slot = route_tables(destination, dest_count)
    serial = jnp.arange(dest_count, dtype=jnp.int32)
    outgoing = []
    for source_blocks, stream in zip(blocks, streams):
        picked_index, present = send_index(
            flat_dest, dest_slot, stream * dp_count + dp_index, serial, capacity
        )
        present = present & (group_id == stream)
        picked = jnp.take(source_blocks, picked_index, axis=0).reshape(dest_count * capacity, -1)
        outgoing.append(jnp.where(present[:, None], picked, jnp.zeros_like(picked)))
    packed = jnp.concatenate(outgoing, axis=1)
    spare_rows = jnp.zeros_like(packed)
    moved_rows = lax.all_to_all(
        jnp.concatenate([spare_rows, packed], axis=0),
        ("group", "dp"),
        split_axis=0,
        concat_axis=0,
        tiled=True,
    )
    arrived = moved_rows[: dest_count * capacity]
    my_index = (group_id - 2) * dp_count + dp_index
    on_backbone = group_id >= 2
    block_count = flat_dest.shape[0]
    source_slot = jnp.arange(block_count, dtype=jnp.int32) // BLOCKS * capacity + dest_slot
    results = []
    offset = 0
    for source_blocks, stream in zip(blocks, streams):
        slot_width = source_blocks[0].size
        columns = arrived[:, offset : offset + slot_width]
        offset = offset + slot_width
        wanted = stream * (BLOCKS // 2) + jnp.arange(BLOCKS // 2, dtype=jnp.int32)
        matches = (flat_dest[None, :] == my_index) & (dest_rank[None, :] == wanted[:, None])
        picked_index = jnp.sum(matches.astype(jnp.int32) * source_slot[None, :], axis=1)
        taken_rows = jnp.take(columns, picked_index, axis=0)
        taken_rows = jnp.where(on_backbone, taken_rows, jnp.zeros_like(taken_rows))
        results.append(taken_rows.reshape((wanted.shape[0],) + source_blocks.shape[1:]))
    return results


def project(audio_rows, image_rows, audio_active, image_active, audio_proj, image_proj):

    def folder(row_block, active, running, shard_part):
        return lax.cond(
            active,
            lambda inner: jnp.dot(row_block, shard_part, preferred_element_type=jnp.float32),
            lambda inner: inner,
            running,
        )

    audio_start = jnp.zeros((audio_rows.shape[0], audio_proj.shape[1]), jnp.float32)
    image_start = jnp.zeros((image_rows.shape[0], image_proj.shape[1]), jnp.float32)
    audio_out = folder(
        audio_rows, audio_active, audio_start, lax.all_gather(audio_proj, "dp", axis=0, tiled=True)
    )
    image_out = folder(
        image_rows, image_active, image_start, lax.all_gather(image_proj, "dp", axis=0, tiled=True)
    )
    return (audio_out, image_out)


def shards_general(
    audio_states,
    image_states,
    audio_gain,
    image_gain,
    audio_proj,
    image_proj,
    block_rows,
    destination,
    input_gain,
    kv_weight,
):
    group_id = lax.axis_index("group")
    dp_index = lax.axis_index("dp")
    mp_index = lax.axis_index("mp")
    mp_count = lax.axis_size("mp")
    share = BLOCK // mp_count
    row_ids = mp_index * share + jnp.arange(share, dtype=jnp.int32)

    def encode(states, gain_vec, stream):
        limits = lax.dynamic_index_in_dim(block_rows[stream], dp_index, 0, keepdims=False)
        keep_rows = (row_ids[None, :] < limits[:, None]).astype(jnp.float32)
        normed = layer_norm(states[0], gain_vec).reshape(BLOCKS, share, -1)
        return (normed * keep_rows[:, :, None]).astype(jnp.bfloat16)

    audio_normed = encode(audio_states, audio_gain, 0)
    image_normed = encode(image_states, image_gain, 1)
    on_backbone = group_id >= 2
    audio_part, image_part = route_blocks(
        (audio_normed, image_normed), (0, 1), destination, group_id, dp_index
    )
    audio_full, image_full = (
        lax.all_gather(audio_part, "mp", axis=1, tiled=True),
        lax.all_gather(image_part, "mp", axis=1, tiled=True),
    )
    audio_out, image_out = project(
        audio_full.reshape(-1, audio_full.shape[2]),
        image_full.reshape(-1, image_full.shape[2]),
        on_backbone,
        on_backbone,
        audio_proj,
        image_proj,
    )
    arrived = (
        jnp.concatenate([audio_out, image_out], axis=0)
        .astype(jnp.bfloat16)
        .reshape(BLOCKS, BLOCK, -1)
    )
    token_rows = arrived.reshape(BLOCKS * BLOCK, -1)
    tokens = token_rows.astype(jnp.float32)
    squares = lax.psum(jnp.sum(tokens * tokens, axis=1), "mp")
    scaled = (tokens * input_gain).astype(jnp.bfloat16)
    partial_value = jnp.dot(scaled, kv_weight, preferred_element_type=jnp.float32)
    summed = lax.psum_scatter(partial_value, "mp", scatter_dimension=1, tiled=True)
    full_width = tokens.shape[1] * mp_count
    result = summed * lax.rsqrt(squares / full_width + EPS_ROOT)[:, None]
    return (result.astype(jnp.bfloat16)[None], token_rows[None])


MIB = 1 << 20


def smem():
    return pl.BlockSpec(memory_space=pltpu.SMEM)


def vmem():
    return pl.BlockSpec(memory_space=pltpu.VMEM)


def hbm():
    return pl.BlockSpec(memory_space=pltpu.HBM)


def in_hbm(arrays):
    return [pltpu.with_memory_space_constraint(x, pltpu.HBM) for x in arrays]


def limits_of(mib, flops=0):
    return dict(
        compiler_params=pltpu.CompilerParams(vmem_limit_bytes=mib * MIB),
        cost_estimate=pl.CostEstimate(flops=flops, transcendentals=0, bytes_accessed=0),
    )


def encode_kernel(dp_count, meta, dest, limits, *refs):
    group, dp, mp = meta[0], meta[1], meta[2]
    targets = 2 * dp_count
    inputs, messages, scratch = refs[:4], refs[4 : 4 + 2 * targets], refs[4 + 2 * targets :]
    routes, lives, *places, sems = scratch
    for stream in range(2):
        states, gain = places[2 * stream : 2 * stream + 2]
        outs = messages[stream * targets : (stream + 1) * targets]
        share = states.shape[1] // BLOCKS
        half = outs[0].shape[1]

        @pl.when(group == stream)
        def _():
            copies = [
                pltpu.make_async_copy(source, place, sems.at[i])
                for i, (source, place) in enumerate(
                    (
                        (dest, routes),
                        (limits, lives),
                        (inputs[2 * stream], states),
                        (inputs[2 * stream + 1], gain),
                    )
                )
            ]
            for copy in copies:
                copy.start()
            for copy in copies:
                copy.wait()
            scale = gain[...].reshape(1, -1)
            for target in range(targets):
                block = jnp.int32(0)
                for b in range(BLOCKS):
                    block = jnp.where(routes[stream, dp, b] == target, b, block)
                limit = lives[stream, dp, block]
                start = pl.multiple_of(block * share, share)
                values = states[0, pl.ds(start, share), :].astype(jnp.float32)
                center = values - jnp.mean(values, axis=-1, keepdims=True)
                spread = jnp.mean(center * center, axis=-1, keepdims=True)
                normed = center * lax.rsqrt(spread + EPS_LAYER) * scale
                row = mp * share + lax.broadcasted_iota(jnp.int32, normed.shape, 0)
                normed = jnp.where(row < limit, normed, 0.0).astype(jnp.bfloat16)
                c, home = target // dp_count, target % dp_count
                for k in range(dp_count):
                    place = 0 if home == k else 1
                    outs[c * dp_count + k][place * share : (place + 1) * share, :] = normed[
                        :, k * half : (k + 1) * half
                    ]


def encode(dp_count, meta, dest, limits, streams):
    arguments, shapes = [], []
    scratch = [pltpu.SMEM(dest.shape, jnp.int32), pltpu.SMEM(limits.shape, jnp.int32)]
    for states, gain, _ in streams:
        _, rows, width = states.shape
        arguments += [states, gain]
        scratch += [pltpu.VMEM(states.shape, states.dtype), pltpu.VMEM(gain.shape, gain.dtype)]
        shape = jax.ShapeDtypeStruct((2 * rows // BLOCKS, width // dp_count), jnp.bfloat16)
        shapes += [shape] * (2 * dp_count)
    return pl.pallas_call(
        functools.partial(encode_kernel, dp_count),
        out_shape=shapes,
        in_specs=[smem()] + [hbm()] * (2 + len(arguments)),
        out_specs=[vmem()] * len(shapes),
        scratch_shapes=scratch + [pltpu.SemaphoreType.DMA((4,))],
        name="encode",
        **limits_of(8, 1 << 28),
    )(meta, *in_hbm([dest, limits, *arguments]))


def fetch_kernel(cuts, *refs):
    count = len(cuts)
    sources, places, sems = refs[:count], refs[count : 2 * count], refs[2 * count]
    copies = []
    for source, place, pieces in zip(sources, places, cuts):
        depth = source.shape[0] // pieces
        for i in range(pieces):
            part = pl.ds(i * depth, depth)
            copies.append(
                pltpu.make_async_copy(source.at[part], place.at[part], sems.at[len(copies)])
            )
    for copy in copies:
        copy.start()
    for copy in copies:
        copy.wait()


def fetch(weights, cuts):
    return pl.pallas_call(
        functools.partial(fetch_kernel, cuts),
        out_shape=[pltpu.VMEM(x.shape, x.dtype) for x in weights],
        in_specs=[hbm()] * len(weights),
        out_specs=[vmem()] * len(weights),
        scratch_shapes=[pltpu.SemaphoreType.DMA((sum(cuts),))],
        name="fetch",
        **limits_of(12, 1 << 28),
    )(*in_hbm(weights))


def project_kernel(mp_count, tile, meta, *refs):
    pieces, weight, keep, send, rows = refs[:mp_count], *refs[mp_count:]
    share = pieces[0].shape[0] // 2
    block = share * mp_count
    for shift in range(mp_count):
        source = lax.rem(meta[2] + (mp_count - shift), mp_count)
        start = pl.multiple_of(source * share, share)
        rows[pl.ds(start, share), :] = pieces[shift][:share, :]
        rows[pl.ds(block + start, share), :] = pieces[shift][share:, :]
    for first in range(0, weight.shape[1], tile):
        out = jnp.dot(
            rows[...], weight[:, first : first + tile], preferred_element_type=jnp.float32
        )
        keep[:, first : first + tile] = out[:block]
        send[:, first : first + tile] = out[block:].astype(jnp.bfloat16)


def project_rows(mp_count, meta, pieces, weight, tile):
    depth, width = weight.shape
    rows = pieces[0].shape[0] * mp_count
    return pl.pallas_call(
        functools.partial(project_kernel, mp_count, tile),
        out_shape=[
            jax.ShapeDtypeStruct((rows // 2, width), jnp.float32),
            jax.ShapeDtypeStruct((rows // 2, width), jnp.bfloat16),
        ],
        in_specs=[smem()] + [vmem()] * (mp_count + 1),
        out_specs=[vmem()] * 2,
        scratch_shapes=[pltpu.VMEM((rows, depth), jnp.bfloat16)],
        name="project",
        **limits_of(12, 2 * rows * depth * width),
    )(meta, *pieces, weight)


def heads_kernel(mp_count, meta, keep, other, gain, weight, tokens, own, *rest):
    sends, scaled = rest[:-1], rest[-1]
    rows, tile = own.shape[0] - 8, own.shape[1]
    rounded = (keep[...] + other[...].astype(jnp.float32)).astype(jnp.bfloat16)
    tokens[...] = rounded
    values = rounded.astype(jnp.float32)
    scaled[...] = (values * gain[...].reshape(1, -1)).astype(jnp.bfloat16)
    total = jnp.sum(values * values, axis=1, keepdims=True)
    turned = jnp.transpose(jnp.broadcast_to(total, (rows, 128)))[:8]
    high = turned.astype(jnp.bfloat16).astype(jnp.float32)
    line = lax.broadcasted_iota(jnp.int32, turned.shape, 0)
    packed = jnp.where(line == 0, high, jnp.where(line == 1, turned - high, 0.0))
    packed = jnp.concatenate([packed] + [jnp.zeros((8, tile - rows), jnp.float32)], axis=1)
    for shift in list(range(1, mp_count)) + [0]:
        chunk = lax.rem(meta[2] + shift, mp_count)
        columns = pl.ds(pl.multiple_of(chunk * tile, tile), tile)
        out = jnp.dot(scaled[...], weight[:, columns], preferred_element_type=jnp.float32)
        if shift:
            block = jnp.concatenate([out, packed], axis=0)
            sends[shift - 1][...] = block.astype(jnp.bfloat16)
        else:
            own[:rows, :] = out
            own[rows:, :] = packed


def heads(mp_count, meta, keep, other, gain, weight):
    rows, width = keep.shape
    tile = weight.shape[1] // mp_count
    return pl.pallas_call(
        functools.partial(heads_kernel, mp_count),
        in_specs=[smem()] + [vmem()] * 4,
        out_specs=[vmem()] * (1 + mp_count),
        scratch_shapes=[pltpu.VMEM((rows, width), jnp.bfloat16)],
        out_shape=[
            jax.ShapeDtypeStruct((rows, width), jnp.bfloat16),
            jax.ShapeDtypeStruct((rows + 8, tile), jnp.float32),
        ]
        + [jax.ShapeDtypeStruct((rows + 8, tile), jnp.bfloat16)] * (mp_count - 1),
        name="heads",
        **limits_of(14, 2 * rows * width * weight.shape[1]),
    )(meta, keep, other, gain, weight)


def finish_kernel(full_width, own, *refs):
    parts, result = refs[:-1], refs[-1]
    rows = result.shape[0]
    total = own[...]
    for part in parts:
        total = total + part[...].astype(jnp.float32)
    square = total[rows : rows + 1, :rows] + total[rows + 1 : rows + 2, :rows]
    scale = lax.rsqrt(square / full_width + EPS_ROOT)
    column = jnp.transpose(jnp.broadcast_to(scale, (128, rows)))[:, :1]
    result[...] = (total[:rows] * column).astype(jnp.bfloat16)


def finish(full_width, own, parts):
    rows, tile = own.shape
    return pl.pallas_call(
        functools.partial(finish_kernel, full_width),
        out_shape=jax.ShapeDtypeStruct((rows - 8, tile), jnp.bfloat16),
        in_specs=[vmem()] * (1 + len(parts)),
        out_specs=vmem(),
        name="finish",
        **limits_of(4, 1 << 26),
    )(own, *parts)


def shards_direct(
    audio_states,
    image_states,
    audio_gain,
    image_gain,
    audio_proj,
    image_proj,
    block_rows,
    destination,
    input_gain,
    kv_weight,
):
    group = lax.axis_index("group")
    dp = lax.axis_index("dp")
    mp = lax.axis_index("mp")
    dp_count = lax.axis_size("dp")
    mp_count = lax.axis_size("mp")
    meta = jnp.stack([group, dp, mp]).astype(jnp.int32)
    rings = [[(i, (i + shift) % mp_count) for i in range(mp_count)] for shift in range(mp_count)]
    swap = [(i, (i + 1) % dp_count) for i in range(dp_count)]
    up = [(0, 2), (1, 3)]
    on_backbone = group >= 2
    mine = lax.rem(group, 2) * dp_count + dp
    full_width = input_gain.shape[0] * mp_count
    targets = 2 * dp_count
    streams = (
        (audio_states, audio_gain, audio_proj),
        (image_states, image_gain, image_proj),
    )

    messages = encode(dp_count, meta, destination, block_rows, streams)
    gathered = []
    for stream in range(2):
        piece = None
        for index in range(targets):
            c, k = index // dp_count, index % dp_count
            pairs = [(stream * dp_count + d, (2 * d + c) * dp_count + k) for d in range(dp_count)]
            moved = lax.ppermute(messages[stream * targets + index], ("group", "dp"), pairs)
            piece = moved if piece is None else jnp.where(mine == index, moved, piece)
        pieces = [piece]
        for shift in range(1, mp_count):
            pieces.append(lax.ppermute(piece, "mp", rings[shift]))
        gathered.append(pieces)
    weights = fetch([audio_proj, image_proj], (2, 5))
    partial, others = [], []
    for stream, proj in enumerate(weights):
        partial.append(project_rows(mp_count, meta, gathered[stream], proj, 512))
        others.append(lax.ppermute(partial[stream][1], "dp", swap))
    row_parts, head_parts = [], []
    for stream in range(2):
        tokens, own, *sends = heads(
            mp_count, meta, partial[stream][0], others[stream], input_gain, kv_weight
        )
        sums = []
        for shift, part in enumerate(sends, 1):
            sums.append(lax.ppermute(part, "mp", rings[shift]))
        row_parts += [lax.ppermute(tokens, "group", up), tokens]
        values = finish(full_width, own, sums)
        head_parts += [lax.ppermute(values, "group", up), values]
    rows_out = jnp.concatenate(row_parts, axis=0)
    rows_out = jnp.where(on_backbone, rows_out, jnp.zeros_like(rows_out))
    heads_out = jnp.concatenate(head_parts, axis=0)
    heads_out = jnp.where(on_backbone, heads_out, jnp.zeros_like(heads_out))
    return (heads_out[None], rows_out[None])


def solution(mesh):
    if 2 * mesh.shape["dp"] != BLOCKS:
        return mapped(shards_general, mesh)
    layer = lambda *inputs: shards_direct(*inputs)
    return mapped(layer, mesh)


def mapped(shards, mesh):
    in_specs = (
        P("group", ("dp", "mp"), None),
        P("group", ("dp", "mp"), None),
        P(),
        P(),
        P("dp", "mp"),
        P("dp", "mp"),
        P(),
        P(),
        P("mp"),
        P("mp", None),
    )
    out_specs = (P("group", "dp", "mp"), P("group", "dp", "mp"))
    return jax.shard_map(shards, mesh=mesh, in_specs=in_specs, out_specs=out_specs, check_vma=False)
```

```python
import functools

import jax
import jax.numpy as jnp
from jax import lax
from jax.experimental import pallas as pl
from jax.experimental.pallas import tpu as pltpu
from jax.sharding import PartitionSpec as P


BLOCK = 128
BLOCKS = 4


EPS_LAYER = 1e-05
EPS_ROOT = 1e-06


def layer_norm(values_in, gain_vec):
    values = values_in.astype(jnp.float32)
    center = values - jnp.mean(values, axis=-1, keepdims=True)
    spread = jnp.mean(center * center, axis=-1, keepdims=True)
    return center * lax.rsqrt(spread + EPS_LAYER) * gain_vec


def route_tables(destination, dest_count):
    flat_dest = destination.reshape(-1)
    hit_table = (flat_dest[:, None] == jnp.arange(dest_count, dtype=jnp.int32)[None, :]).astype(
        jnp.int32
    )
    dest_rank = jnp.sum((jnp.cumsum(hit_table, axis=0) - 1) * hit_table, axis=1)
    per_source = hit_table.reshape(-1, BLOCKS, dest_count)
    dest_slot = jnp.sum((jnp.cumsum(per_source, axis=1) - 1) * per_source, axis=2).reshape(-1)
    return (flat_dest, dest_rank, dest_slot)


def send_index(flat_dest, dest_slot, source, targets, capacity):
    row_dest = lax.dynamic_slice_in_dim(flat_dest, source * BLOCKS, BLOCKS)
    row_slot = lax.dynamic_slice_in_dim(dest_slot, source * BLOCKS, BLOCKS)
    wanted_slot = jnp.arange(capacity, dtype=jnp.int32)
    matches = (row_dest[None, None, :] == targets[:, None, None]) & (
        row_slot[None, None, :] == wanted_slot[None, :, None]
    )
    block_ids = jnp.arange(BLOCKS, dtype=jnp.int32)
    picked_index = jnp.sum(matches.astype(jnp.int32) * block_ids[None, None, :], axis=2).reshape(-1)
    present = jnp.any(matches, axis=2).reshape(-1)
    return (picked_index, present)


def route_blocks(blocks, streams, destination, group_id, dp_index):
    dp_count = lax.axis_size("dp")
    dest_count = 2 * dp_count
    capacity = BLOCKS // 4
    flat_dest, dest_rank, dest_slot = route_tables(destination, dest_count)
    serial = jnp.arange(dest_count, dtype=jnp.int32)
    outgoing = []
    for source_blocks, stream in zip(blocks, streams):
        picked_index, present = send_index(
            flat_dest, dest_slot, stream * dp_count + dp_index, serial, capacity
        )
        present = present & (group_id == stream)
        picked = jnp.take(source_blocks, picked_index, axis=0).reshape(dest_count * capacity, -1)
        outgoing.append(jnp.where(present[:, None], picked, jnp.zeros_like(picked)))
    packed = jnp.concatenate(outgoing, axis=1)
    spare_rows = jnp.zeros_like(packed)
    moved_rows = lax.all_to_all(
        jnp.concatenate([spare_rows, packed], axis=0),
        ("group", "dp"),
        split_axis=0,
        concat_axis=0,
        tiled=True,
    )
    arrived = moved_rows[: dest_count * capacity]
    my_index = (group_id - 2) * dp_count + dp_index
    on_backbone = group_id >= 2
    block_count = flat_dest.shape[0]
    source_slot = jnp.arange(block_count, dtype=jnp.int32) // BLOCKS * capacity + dest_slot
    results = []
    offset = 0
    for source_blocks, stream in zip(blocks, streams):
        slot_width = source_blocks[0].size
        columns = arrived[:, offset : offset + slot_width]
        offset = offset + slot_width
        wanted = stream * (BLOCKS // 2) + jnp.arange(BLOCKS // 2, dtype=jnp.int32)
        matches = (flat_dest[None, :] == my_index) & (dest_rank[None, :] == wanted[:, None])
        picked_index = jnp.sum(matches.astype(jnp.int32) * source_slot[None, :], axis=1)
        taken_rows = jnp.take(columns, picked_index, axis=0)
        taken_rows = jnp.where(on_backbone, taken_rows, jnp.zeros_like(taken_rows))
        results.append(taken_rows.reshape((wanted.shape[0],) + source_blocks.shape[1:]))
    return results


def project(audio_rows, image_rows, audio_active, image_active, audio_proj, image_proj):

    def folder(row_block, active, running, shard_part):
        return lax.cond(
            active,
            lambda inner: jnp.dot(row_block, shard_part, preferred_element_type=jnp.float32),
            lambda inner: inner,
            running,
        )

    audio_start = jnp.zeros((audio_rows.shape[0], audio_proj.shape[1]), jnp.float32)
    image_start = jnp.zeros((image_rows.shape[0], image_proj.shape[1]), jnp.float32)
    audio_out = folder(
        audio_rows, audio_active, audio_start, lax.all_gather(audio_proj, "dp", axis=0, tiled=True)
    )
    image_out = folder(
        image_rows, image_active, image_start, lax.all_gather(image_proj, "dp", axis=0, tiled=True)
    )
    return (audio_out, image_out)


def shards_general(
    audio_states,
    image_states,
    audio_gain,
    image_gain,
    audio_proj,
    image_proj,
    block_rows,
    destination,
    input_gain,
    kv_weight,
):
    group_id = lax.axis_index("group")
    dp_index = lax.axis_index("dp")
    mp_index = lax.axis_index("mp")
    mp_count = lax.axis_size("mp")
    share = BLOCK // mp_count
    row_ids = mp_index * share + jnp.arange(share, dtype=jnp.int32)

    def encode(states, gain_vec, stream):
        limits = lax.dynamic_index_in_dim(block_rows[stream], dp_index, 0, keepdims=False)
        keep_rows = (row_ids[None, :] < limits[:, None]).astype(jnp.float32)
        normed = layer_norm(states[0], gain_vec).reshape(BLOCKS, share, -1)
        return (normed * keep_rows[:, :, None]).astype(jnp.bfloat16)

    audio_normed = encode(audio_states, audio_gain, 0)
    image_normed = encode(image_states, image_gain, 1)
    on_backbone = group_id >= 2
    audio_part, image_part = route_blocks(
        (audio_normed, image_normed), (0, 1), destination, group_id, dp_index
    )
    audio_full, image_full = (
        lax.all_gather(audio_part, "mp", axis=1, tiled=True),
        lax.all_gather(image_part, "mp", axis=1, tiled=True),
    )
    audio_out, image_out = project(
        audio_full.reshape(-1, audio_full.shape[2]),
        image_full.reshape(-1, image_full.shape[2]),
        on_backbone,
        on_backbone,
        audio_proj,
        image_proj,
    )
    arrived = (
        jnp.concatenate([audio_out, image_out], axis=0)
        .astype(jnp.bfloat16)
        .reshape(BLOCKS, BLOCK, -1)
    )
    token_rows = arrived.reshape(BLOCKS * BLOCK, -1)
    tokens = token_rows.astype(jnp.float32)
    squares = lax.psum(jnp.sum(tokens * tokens, axis=1), "mp")
    scaled = (tokens * input_gain).astype(jnp.bfloat16)
    partial_value = jnp.dot(scaled, kv_weight, preferred_element_type=jnp.float32)
    summed = lax.psum_scatter(partial_value, "mp", scatter_dimension=1, tiled=True)
    full_width = tokens.shape[1] * mp_count
    result = summed * lax.rsqrt(squares / full_width + EPS_ROOT)[:, None]
    return (result.astype(jnp.bfloat16)[None], token_rows[None])


MIB = 1 << 20


def smem():
    return pl.BlockSpec(memory_space=pltpu.SMEM)


def vmem():
    return pl.BlockSpec(memory_space=pltpu.VMEM)


def hbm():
    return pl.BlockSpec(memory_space=pltpu.HBM)


def in_hbm(arrays):
    return [pltpu.with_memory_space_constraint(x, pltpu.HBM) for x in arrays]


def limits_of(mib, flops=0):
    return dict(
        compiler_params=pltpu.CompilerParams(vmem_limit_bytes=mib * MIB),
        cost_estimate=pl.CostEstimate(flops=flops, transcendentals=0, bytes_accessed=0),
    )


def encode_kernel(dp_count, meta, dest, limits, *refs):
    group, dp, mp = meta[0], meta[1], meta[2]
    targets = 2 * dp_count
    inputs, messages, scratch = refs[:4], refs[4 : 4 + 2 * targets], refs[4 + 2 * targets :]
    routes, lives, *places, sems = scratch
    for stream in range(2):
        states, gain = places[2 * stream : 2 * stream + 2]
        outs = messages[stream * targets : (stream + 1) * targets]
        share = states.shape[1] // BLOCKS
        half = outs[0].shape[1]

        @pl.when(group == stream)
        def _():
            copies = [
                pltpu.make_async_copy(source, place, sems.at[i])
                for i, (source, place) in enumerate(
                    (
                        (dest, routes),
                        (limits, lives),
                        (inputs[2 * stream], states),
                        (inputs[2 * stream + 1], gain),
                    )
                )
            ]
            for copy in copies:
                copy.start()
            for copy in copies:
                copy.wait()
            scale = gain[...].reshape(1, -1)
            for target in range(targets):
                block = jnp.int32(0)
                for b in range(BLOCKS):
                    block = jnp.where(routes[stream, dp, b] == target, b, block)
                limit = lives[stream, dp, block]
                start = pl.multiple_of(block * share, share)
                values = states[0, pl.ds(start, share), :].astype(jnp.float32)
                center = values - jnp.mean(values, axis=-1, keepdims=True)
                spread = jnp.mean(center * center, axis=-1, keepdims=True)
                normed = center * lax.rsqrt(spread + EPS_LAYER) * scale
                row = mp * share + lax.broadcasted_iota(jnp.int32, normed.shape, 0)
                normed = jnp.where(row < limit, normed, 0.0).astype(jnp.bfloat16)
                c, home = target // dp_count, target % dp_count
                for k in range(dp_count):
                    place = 0 if home == k else 1
                    outs[c * dp_count + k][place * share : (place + 1) * share, :] = normed[
                        :, k * half : (k + 1) * half
                    ]


def encode(dp_count, meta, dest, limits, streams):
    arguments, shapes = [], []
    scratch = [pltpu.SMEM(dest.shape, jnp.int32), pltpu.SMEM(limits.shape, jnp.int32)]
    for states, gain, _ in streams:
        _, rows, width = states.shape
        arguments += [states, gain]
        scratch += [pltpu.VMEM(states.shape, states.dtype), pltpu.VMEM(gain.shape, gain.dtype)]
        shape = jax.ShapeDtypeStruct((2 * rows // BLOCKS, width // dp_count), jnp.bfloat16)
        shapes += [shape] * (2 * dp_count)
    return pl.pallas_call(
        functools.partial(encode_kernel, dp_count),
        out_shape=shapes,
        in_specs=[smem()] + [hbm()] * (2 + len(arguments)),
        out_specs=[vmem()] * len(shapes),
        scratch_shapes=scratch + [pltpu.SemaphoreType.DMA((4,))],
        name="encode",
        **limits_of(8, 1 << 28),
    )(meta, *in_hbm([dest, limits, *arguments]))


def fetch_kernel(cuts, *refs):
    count = len(cuts)
    sources, places, sems = refs[:count], refs[count : 2 * count], refs[2 * count]
    copies = []
    for source, place, pieces in zip(sources, places, cuts):
        depth = source.shape[0] // pieces
        for i in range(pieces):
            part = pl.ds(i * depth, depth)
            copies.append(
                pltpu.make_async_copy(source.at[part], place.at[part], sems.at[len(copies)])
            )
    for copy in copies:
        copy.start()
    for copy in copies:
        copy.wait()


def fetch(weights, cuts):
    return pl.pallas_call(
        functools.partial(fetch_kernel, cuts),
        out_shape=[pltpu.VMEM(x.shape, x.dtype) for x in weights],
        in_specs=[hbm()] * len(weights),
        out_specs=[vmem()] * len(weights),
        scratch_shapes=[pltpu.SemaphoreType.DMA((sum(cuts),))],
        name="fetch",
        **limits_of(12, 1 << 28),
    )(*in_hbm(weights))


def project_kernel(mp_count, tile, meta, *refs):
    pieces, weight, keep, send, rows = refs[:mp_count], *refs[mp_count:]
    share = pieces[0].shape[0] // 2
    block = share * mp_count
    for shift in range(mp_count):
        source = lax.rem(meta[2] + (mp_count - shift), mp_count)
        start = pl.multiple_of(source * share, share)
        rows[pl.ds(start, share), :] = pieces[shift][:share, :]
        rows[pl.ds(block + start, share), :] = pieces[shift][share:, :]
    for first in range(0, weight.shape[1], tile):
        out = jnp.dot(
            rows[...], weight[:, first : first + tile], preferred_element_type=jnp.float32
        )
        keep[:, first : first + tile] = out[:block]
        send[:, first : first + tile] = out[block:].astype(jnp.bfloat16)


def project_rows(mp_count, meta, pieces, weight, tile):
    depth, width = weight.shape
    rows = pieces[0].shape[0] * mp_count
    return pl.pallas_call(
        functools.partial(project_kernel, mp_count, tile),
        out_shape=[
            jax.ShapeDtypeStruct((rows // 2, width), jnp.float32),
            jax.ShapeDtypeStruct((rows // 2, width), jnp.bfloat16),
        ],
        in_specs=[smem()] + [vmem()] * (mp_count + 1),
        out_specs=[vmem()] * 2,
        scratch_shapes=[pltpu.VMEM((rows, depth), jnp.bfloat16)],
        name="project",
        **limits_of(12, 2 * rows * depth * width),
    )(meta, *pieces, weight)


def heads_kernel(mp_count, meta, keep, other, gain, weight, tokens, own, *rest):
    sends, scaled = rest[:-1], rest[-1]
    rows, tile = own.shape[0] - 8, own.shape[1]
    rounded = (keep[...] + other[...].astype(jnp.float32)).astype(jnp.bfloat16)
    tokens[...] = rounded
    values = rounded.astype(jnp.float32)
    scaled[...] = (values * gain[...].reshape(1, -1)).astype(jnp.bfloat16)
    total = jnp.sum(values * values, axis=1, keepdims=True)
    turned = jnp.transpose(jnp.broadcast_to(total, (rows, 128)))[:8]
    high = turned.astype(jnp.bfloat16).astype(jnp.float32)
    line = lax.broadcasted_iota(jnp.int32, turned.shape, 0)
    packed = jnp.where(line == 0, high, jnp.where(line == 1, turned - high, 0.0))
    packed = jnp.concatenate([packed] + [jnp.zeros((8, tile - rows), jnp.float32)], axis=1)
    for shift in list(range(1, mp_count)) + [0]:
        chunk = lax.rem(meta[2] + shift, mp_count)
        columns = pl.ds(pl.multiple_of(chunk * tile, tile), tile)
        out = jnp.dot(scaled[...], weight[:, columns], preferred_element_type=jnp.float32)
        if shift:
            block = jnp.concatenate([out, packed], axis=0)
            sends[shift - 1][...] = block.astype(jnp.bfloat16)
        else:
            own[:rows, :] = out
            own[rows:, :] = packed


def heads(mp_count, meta, keep, other, gain, weight):
    rows, width = keep.shape
    tile = weight.shape[1] // mp_count
    return pl.pallas_call(
        functools.partial(heads_kernel, mp_count),
        in_specs=[smem()] + [vmem()] * 4,
        out_specs=[vmem()] * (1 + mp_count),
        scratch_shapes=[pltpu.VMEM((rows, width), jnp.bfloat16)],
        out_shape=[
            jax.ShapeDtypeStruct((rows, width), jnp.bfloat16),
            jax.ShapeDtypeStruct((rows + 8, tile), jnp.float32),
        ]
        + [jax.ShapeDtypeStruct((rows + 8, tile), jnp.bfloat16)] * (mp_count - 1),
        name="heads",
        **limits_of(14, 2 * rows * width * weight.shape[1]),
    )(meta, keep, other, gain, weight)


def finish_kernel(full_width, own, *refs):
    parts, result = refs[:-1], refs[-1]
    rows = result.shape[0]
    total = own[...]
    for part in parts:
        total = total + part[...].astype(jnp.float32)
    square = total[rows : rows + 1, :rows] + total[rows + 1 : rows + 2, :rows]
    scale = lax.rsqrt(square / full_width + EPS_ROOT)
    column = jnp.transpose(jnp.broadcast_to(scale, (128, rows)))[:, :1]
    result[...] = (total[:rows] * column).astype(jnp.bfloat16)


def finish(full_width, own, parts):
    rows, tile = own.shape
    return pl.pallas_call(
        functools.partial(finish_kernel, full_width),
        out_shape=jax.ShapeDtypeStruct((rows - 8, tile), jnp.bfloat16),
        in_specs=[vmem()] * (1 + len(parts)),
        out_specs=vmem(),
        name="finish",
        **limits_of(4, 1 << 26),
    )(own, *parts)


def shards_direct(
    audio_states,
    image_states,
    audio_gain,
    image_gain,
    audio_proj,
    image_proj,
    block_rows,
    destination,
    input_gain,
    kv_weight,
):
    group = lax.axis_index("group")
    dp = lax.axis_index("dp")
    mp = lax.axis_index("mp")
    dp_count = lax.axis_size("dp")
    mp_count = lax.axis_size("mp")
    meta = jnp.stack([group, dp, mp]).astype(jnp.int32)
    rings = [[(i, (i + shift) % mp_count) for i in range(mp_count)] for shift in range(mp_count)]
    swap = [(i, (i + 1) % dp_count) for i in range(dp_count)]
    up = [(0, 2), (1, 3)]
    on_backbone = group >= 2
    mine = lax.rem(group, 2) * dp_count + dp
    full_width = input_gain.shape[0] * mp_count
    targets = 2 * dp_count
    streams = (
        (audio_states, audio_gain, audio_proj),
        (image_states, image_gain, image_proj),
    )

    messages = encode(dp_count, meta, destination, block_rows, streams)
    gathered = []
    for stream in range(2):
        piece = None
        for index in range(targets):
            c, k = index // dp_count, index % dp_count
            pairs = [(stream * dp_count + d, (2 * d + c) * dp_count + k) for d in range(dp_count)]
            moved = lax.ppermute(messages[stream * targets + index], ("group", "dp"), pairs)
            piece = moved if piece is None else jnp.where(mine == index, moved, piece)
        pieces = [piece]
        for shift in range(1, mp_count):
            pieces.append(lax.ppermute(piece, "mp", rings[shift]))
        gathered.append(pieces)
    partial, others = [], []
    for stream, (_, _, proj) in enumerate(streams):
        wanted = [proj] if stream == 0 else [proj, kv_weight]
        proj, *heads_weight = fetch(wanted, (4,) * len(wanted))
        partial.append(project_rows(mp_count, meta, gathered[stream], proj, 512))
        others.append(lax.ppermute(partial[stream][1], "dp", swap))
    row_parts, head_parts = [], []
    for stream in range(2):
        tokens, own, *sends = heads(
            mp_count, meta, partial[stream][0], others[stream], input_gain, heads_weight[0]
        )
        sums = []
        for shift, part in enumerate(sends, 1):
            sums.append(lax.ppermute(part, "mp", rings[shift]))
        row_parts += [lax.ppermute(tokens, "group", up), tokens]
        values = finish(full_width, own, sums)
        head_parts += [lax.ppermute(values, "group", up), values]
    rows_out = jnp.concatenate(row_parts, axis=0)
    rows_out = jnp.where(on_backbone, rows_out, jnp.zeros_like(rows_out))
    heads_out = jnp.concatenate(head_parts, axis=0)
    heads_out = jnp.where(on_backbone, heads_out, jnp.zeros_like(heads_out))
    return (heads_out[None], rows_out[None])


def solution(mesh):
    if 2 * mesh.shape["dp"] != BLOCKS:
        return mapped(shards_general, mesh)
    layer = lambda *inputs: shards_direct(*inputs)
    return mapped(layer, mesh)


def mapped(shards, mesh):
    in_specs = (
        P("group", ("dp", "mp"), None),
        P("group", ("dp", "mp"), None),
        P(),
        P(),
        P("dp", "mp"),
        P("dp", "mp"),
        P(),
        P(),
        P("mp"),
        P("mp", None),
    )
    out_specs = (P("group", "dp", "mp"), P("group", "dp", "mp"))
    return jax.shard_map(shards, mesh=mesh, in_specs=in_specs, out_specs=out_specs, check_vma=False)
```

```python
import functools

import jax
import jax.numpy as jnp
from jax import lax
from jax.experimental import pallas as pl
from jax.experimental.pallas import tpu as pltpu
from jax.sharding import PartitionSpec as P


BLOCK = 128
BLOCKS = 4


EPS_LAYER = 1e-05
EPS_ROOT = 1e-06


def layer_norm(values_in, gain_vec):
    values = values_in.astype(jnp.float32)
    center = values - jnp.mean(values, axis=-1, keepdims=True)
    spread = jnp.mean(center * center, axis=-1, keepdims=True)
    return center * lax.rsqrt(spread + EPS_LAYER) * gain_vec


def route_tables(destination, dest_count):
    flat_dest = destination.reshape(-1)
    hit_table = (flat_dest[:, None] == jnp.arange(dest_count, dtype=jnp.int32)[None, :]).astype(
        jnp.int32
    )
    dest_rank = jnp.sum((jnp.cumsum(hit_table, axis=0) - 1) * hit_table, axis=1)
    per_source = hit_table.reshape(-1, BLOCKS, dest_count)
    dest_slot = jnp.sum((jnp.cumsum(per_source, axis=1) - 1) * per_source, axis=2).reshape(-1)
    return (flat_dest, dest_rank, dest_slot)


def send_index(flat_dest, dest_slot, source, targets, capacity):
    row_dest = lax.dynamic_slice_in_dim(flat_dest, source * BLOCKS, BLOCKS)
    row_slot = lax.dynamic_slice_in_dim(dest_slot, source * BLOCKS, BLOCKS)
    wanted_slot = jnp.arange(capacity, dtype=jnp.int32)
    matches = (row_dest[None, None, :] == targets[:, None, None]) & (
        row_slot[None, None, :] == wanted_slot[None, :, None]
    )
    block_ids = jnp.arange(BLOCKS, dtype=jnp.int32)
    picked_index = jnp.sum(matches.astype(jnp.int32) * block_ids[None, None, :], axis=2).reshape(-1)
    present = jnp.any(matches, axis=2).reshape(-1)
    return (picked_index, present)


def route_blocks(blocks, streams, destination, group_id, dp_index):
    dp_count = lax.axis_size("dp")
    dest_count = 2 * dp_count
    capacity = BLOCKS // 4
    flat_dest, dest_rank, dest_slot = route_tables(destination, dest_count)
    serial = jnp.arange(dest_count, dtype=jnp.int32)
    outgoing = []
    for source_blocks, stream in zip(blocks, streams):
        picked_index, present = send_index(
            flat_dest, dest_slot, stream * dp_count + dp_index, serial, capacity
        )
        present = present & (group_id == stream)
        picked = jnp.take(source_blocks, picked_index, axis=0).reshape(dest_count * capacity, -1)
        outgoing.append(jnp.where(present[:, None], picked, jnp.zeros_like(picked)))
    packed = jnp.concatenate(outgoing, axis=1)
    spare_rows = jnp.zeros_like(packed)
    moved_rows = lax.all_to_all(
        jnp.concatenate([spare_rows, packed], axis=0),
        ("group", "dp"),
        split_axis=0,
        concat_axis=0,
        tiled=True,
    )
    arrived = moved_rows[: dest_count * capacity]
    my_index = (group_id - 2) * dp_count + dp_index
    on_backbone = group_id >= 2
    block_count = flat_dest.shape[0]
    source_slot = jnp.arange(block_count, dtype=jnp.int32) // BLOCKS * capacity + dest_slot
    results = []
    offset = 0
    for source_blocks, stream in zip(blocks, streams):
        slot_width = source_blocks[0].size
        columns = arrived[:, offset : offset + slot_width]
        offset = offset + slot_width
        wanted = stream * (BLOCKS // 2) + jnp.arange(BLOCKS // 2, dtype=jnp.int32)
        matches = (flat_dest[None, :] == my_index) & (dest_rank[None, :] == wanted[:, None])
        picked_index = jnp.sum(matches.astype(jnp.int32) * source_slot[None, :], axis=1)
        taken_rows = jnp.take(columns, picked_index, axis=0)
        taken_rows = jnp.where(on_backbone, taken_rows, jnp.zeros_like(taken_rows))
        results.append(taken_rows.reshape((wanted.shape[0],) + source_blocks.shape[1:]))
    return results


def project(audio_rows, image_rows, audio_active, image_active, audio_proj, image_proj):

    def folder(row_block, active, running, shard_part):
        return lax.cond(
            active,
            lambda inner: jnp.dot(row_block, shard_part, preferred_element_type=jnp.float32),
            lambda inner: inner,
            running,
        )

    audio_start = jnp.zeros((audio_rows.shape[0], audio_proj.shape[1]), jnp.float32)
    image_start = jnp.zeros((image_rows.shape[0], image_proj.shape[1]), jnp.float32)
    audio_out = folder(
        audio_rows, audio_active, audio_start, lax.all_gather(audio_proj, "dp", axis=0, tiled=True)
    )
    image_out = folder(
        image_rows, image_active, image_start, lax.all_gather(image_proj, "dp", axis=0, tiled=True)
    )
    return (audio_out, image_out)


def shards_general(
    audio_states,
    image_states,
    audio_gain,
    image_gain,
    audio_proj,
    image_proj,
    block_rows,
    destination,
    input_gain,
    kv_weight,
):
    group_id = lax.axis_index("group")
    dp_index = lax.axis_index("dp")
    mp_index = lax.axis_index("mp")
    mp_count = lax.axis_size("mp")
    share = BLOCK // mp_count
    row_ids = mp_index * share + jnp.arange(share, dtype=jnp.int32)

    def encode(states, gain_vec, stream):
        limits = lax.dynamic_index_in_dim(block_rows[stream], dp_index, 0, keepdims=False)
        keep_rows = (row_ids[None, :] < limits[:, None]).astype(jnp.float32)
        normed = layer_norm(states[0], gain_vec).reshape(BLOCKS, share, -1)
        return (normed * keep_rows[:, :, None]).astype(jnp.bfloat16)

    audio_normed = encode(audio_states, audio_gain, 0)
    image_normed = encode(image_states, image_gain, 1)
    on_backbone = group_id >= 2
    audio_part, image_part = route_blocks(
        (audio_normed, image_normed), (0, 1), destination, group_id, dp_index
    )
    audio_full, image_full = (
        lax.all_gather(audio_part, "mp", axis=1, tiled=True),
        lax.all_gather(image_part, "mp", axis=1, tiled=True),
    )
    audio_out, image_out = project(
        audio_full.reshape(-1, audio_full.shape[2]),
        image_full.reshape(-1, image_full.shape[2]),
        on_backbone,
        on_backbone,
        audio_proj,
        image_proj,
    )
    arrived = (
        jnp.concatenate([audio_out, image_out], axis=0)
        .astype(jnp.bfloat16)
        .reshape(BLOCKS, BLOCK, -1)
    )
    token_rows = arrived.reshape(BLOCKS * BLOCK, -1)
    tokens = token_rows.astype(jnp.float32)
    squares = lax.psum(jnp.sum(tokens * tokens, axis=1), "mp")
    scaled = (tokens * input_gain).astype(jnp.bfloat16)
    partial_value = jnp.dot(scaled, kv_weight, preferred_element_type=jnp.float32)
    summed = lax.psum_scatter(partial_value, "mp", scatter_dimension=1, tiled=True)
    full_width = tokens.shape[1] * mp_count
    result = summed * lax.rsqrt(squares / full_width + EPS_ROOT)[:, None]
    return (result.astype(jnp.bfloat16)[None], token_rows[None])


MIB = 1 << 20


def smem():
    return pl.BlockSpec(memory_space=pltpu.SMEM)


def vmem():
    return pl.BlockSpec(memory_space=pltpu.VMEM)


def hbm():
    return pl.BlockSpec(memory_space=pltpu.HBM)


def in_hbm(arrays):
    return [pltpu.with_memory_space_constraint(x, pltpu.HBM) for x in arrays]


def limits_of(mib, flops=0):
    return dict(
        compiler_params=pltpu.CompilerParams(vmem_limit_bytes=mib * MIB),
        cost_estimate=pl.CostEstimate(flops=flops, transcendentals=0, bytes_accessed=0),
    )


def deal_index(stream, c, k, dp_count):
    return (c if stream == 0 else 1 - c) * dp_count + k


def encode_kernel(dp_count, meta, dest, limits, *refs):
    group, dp, mp = meta[0], meta[1], meta[2]
    targets = 2 * dp_count
    inputs, outs, scratch = refs[:4], refs[4 : 4 + targets], refs[4 + targets :]
    routes, lives, *places, sems = scratch
    for stream in range(2):
        states, gain = places[2 * stream : 2 * stream + 2]
        share = states.shape[1] // BLOCKS
        half = states.shape[2] // dp_count

        @pl.when(group == stream)
        def _():
            copies = [
                pltpu.make_async_copy(source, place, sems.at[i])
                for i, (source, place) in enumerate(
                    (
                        (dest, routes),
                        (limits, lives),
                        (inputs[2 * stream], states),
                        (inputs[2 * stream + 1], gain),
                    )
                )
            ]
            for copy in copies:
                copy.start()
            for copy in copies:
                copy.wait()
            scale = gain[...].reshape(1, -1)
            for target in range(targets):
                block = jnp.int32(0)
                for b in range(BLOCKS):
                    block = jnp.where(routes[stream, dp, b] == target, b, block)
                limit = lives[stream, dp, block]
                start = pl.multiple_of(block * share, share)
                values = states[0, pl.ds(start, share), :].astype(jnp.float32)
                center = values - jnp.mean(values, axis=-1, keepdims=True)
                spread = jnp.mean(center * center, axis=-1, keepdims=True)
                normed = center * lax.rsqrt(spread + EPS_LAYER) * scale
                row = mp * share + lax.broadcasted_iota(jnp.int32, normed.shape, 0)
                normed = jnp.where(row < limit, normed, 0.0).astype(jnp.bfloat16)
                c, home = target // dp_count, target % dp_count
                for k in range(dp_count):
                    place = 0 if home == k else 1
                    outs[deal_index(stream, c, k, dp_count)][
                        place * share : (place + 1) * share, :half
                    ] = normed[:, k * half : (k + 1) * half]


def encode(dp_count, meta, dest, limits, streams):
    arguments = []
    scratch = [pltpu.SMEM(dest.shape, jnp.int32), pltpu.SMEM(limits.shape, jnp.int32)]
    for states, gain, _ in streams:
        arguments += [states, gain]
        scratch += [pltpu.VMEM(states.shape, states.dtype), pltpu.VMEM(gain.shape, gain.dtype)]
    rows = streams[0][0].shape[1]
    half = max(states.shape[2] for states, _, _ in streams) // dp_count
    shapes = [jax.ShapeDtypeStruct((2 * rows // BLOCKS, half), jnp.bfloat16)] * (2 * dp_count)
    return pl.pallas_call(
        functools.partial(encode_kernel, dp_count),
        out_shape=shapes,
        in_specs=[smem()] + [hbm()] * (2 + len(arguments)),
        out_specs=[vmem()] * len(shapes),
        scratch_shapes=scratch + [pltpu.SemaphoreType.DMA((4,))],
        name="encode",
        **limits_of(8, 1 << 28),
    )(meta, *in_hbm([dest, limits, *arguments]))


def fetch_kernel(cuts, *refs):
    count = len(cuts)
    sources, places, sems = refs[:count], refs[count : 2 * count], refs[2 * count]
    copies = []
    for source, place, pieces in zip(sources, places, cuts):
        depth = source.shape[0] // pieces
        for i in range(pieces):
            part = pl.ds(i * depth, depth)
            copies.append(
                pltpu.make_async_copy(source.at[part], place.at[part], sems.at[len(copies)])
            )
    for copy in copies:
        copy.start()
    for copy in copies:
        copy.wait()


def fetch(weights, cuts):
    return pl.pallas_call(
        functools.partial(fetch_kernel, cuts),
        out_shape=[pltpu.VMEM(x.shape, x.dtype) for x in weights],
        in_specs=[hbm()] * len(weights),
        out_specs=[vmem()] * len(weights),
        scratch_shapes=[pltpu.SemaphoreType.DMA((sum(cuts),))],
        name="fetch",
        **limits_of(12, 1 << 28),
    )(*in_hbm(weights))


def project_kernel(mp_count, tile, meta, *refs):
    pieces, weight, keep, send, rows = refs[:mp_count], *refs[mp_count:]
    share = pieces[0].shape[0] // 2
    block = share * mp_count
    for shift in range(mp_count):
        source = lax.rem(meta[2] + (mp_count - shift), mp_count)
        start = pl.multiple_of(source * share, share)
        rows[pl.ds(start, share), :] = pieces[shift][:share, :]
        rows[pl.ds(block + start, share), :] = pieces[shift][share:, :]
    for first in range(0, weight.shape[1], tile):
        out = jnp.dot(
            rows[...], weight[:, first : first + tile], preferred_element_type=jnp.float32
        )
        keep[:, first : first + tile] = out[:block]
        send[:, first : first + tile] = out[block:].astype(jnp.bfloat16)


def project_rows(mp_count, meta, pieces, weight, tile):
    depth, width = weight.shape
    rows = pieces[0].shape[0] * mp_count
    return pl.pallas_call(
        functools.partial(project_kernel, mp_count, tile),
        out_shape=[
            jax.ShapeDtypeStruct((rows // 2, width), jnp.float32),
            jax.ShapeDtypeStruct((rows // 2, width), jnp.bfloat16),
        ],
        in_specs=[smem()] + [vmem()] * (mp_count + 1),
        out_specs=[vmem()] * 2,
        scratch_shapes=[pltpu.VMEM((rows, depth), jnp.bfloat16)],
        name="project",
        **limits_of(12, 2 * rows * depth * width),
    )(meta, *pieces, weight)


def heads_kernel(mp_count, meta, keep, other, gain, weight, tokens, own, *rest):
    sends, scaled = rest[:-1], rest[-1]
    rows, tile = own.shape[0] - 8, own.shape[1]
    rounded = (keep[...] + other[...].astype(jnp.float32)).astype(jnp.bfloat16)
    tokens[...] = rounded
    values = rounded.astype(jnp.float32)
    scaled[...] = (values * gain[...].reshape(1, -1)).astype(jnp.bfloat16)
    total = jnp.sum(values * values, axis=1, keepdims=True)
    turned = jnp.transpose(jnp.broadcast_to(total, (rows, 128)))[:8]
    high = turned.astype(jnp.bfloat16).astype(jnp.float32)
    line = lax.broadcasted_iota(jnp.int32, turned.shape, 0)
    packed = jnp.where(line == 0, high, jnp.where(line == 1, turned - high, 0.0))
    packed = jnp.concatenate([packed] + [jnp.zeros((8, tile - rows), jnp.float32)], axis=1)
    for shift in list(range(1, mp_count)) + [0]:
        chunk = lax.rem(meta[2] + shift, mp_count)
        columns = pl.ds(pl.multiple_of(chunk * tile, tile), tile)
        out = jnp.dot(scaled[...], weight[:, columns], preferred_element_type=jnp.float32)
        if shift:
            block = jnp.concatenate([out, packed], axis=0)
            sends[shift - 1][...] = block.astype(jnp.bfloat16)
        else:
            own[:rows, :] = out
            own[rows:, :] = packed


def heads(mp_count, meta, keep, other, gain, weight):
    rows, width = keep.shape
    tile = weight.shape[1] // mp_count
    return pl.pallas_call(
        functools.partial(heads_kernel, mp_count),
        in_specs=[smem()] + [vmem()] * 4,
        out_specs=[vmem()] * (1 + mp_count),
        scratch_shapes=[pltpu.VMEM((rows, width), jnp.bfloat16)],
        out_shape=[
            jax.ShapeDtypeStruct((rows, width), jnp.bfloat16),
            jax.ShapeDtypeStruct((rows + 8, tile), jnp.float32),
        ]
        + [jax.ShapeDtypeStruct((rows + 8, tile), jnp.bfloat16)] * (mp_count - 1),
        name="heads",
        **limits_of(14, 2 * rows * width * weight.shape[1]),
    )(meta, keep, other, gain, weight)


def finish_kernel(full_width, own, *refs):
    parts, result = refs[:-1], refs[-1]
    rows = result.shape[0]
    total = own[...]
    for part in parts:
        total = total + part[...].astype(jnp.float32)
    square = total[rows : rows + 1, :rows] + total[rows + 1 : rows + 2, :rows]
    scale = lax.rsqrt(square / full_width + EPS_ROOT)
    column = jnp.transpose(jnp.broadcast_to(scale, (128, rows)))[:, :1]
    result[...] = (total[:rows] * column).astype(jnp.bfloat16)


def finish(full_width, own, parts):
    rows, tile = own.shape
    return pl.pallas_call(
        functools.partial(finish_kernel, full_width),
        out_shape=jax.ShapeDtypeStruct((rows - 8, tile), jnp.bfloat16),
        in_specs=[vmem()] * (1 + len(parts)),
        out_specs=vmem(),
        name="finish",
        **limits_of(4, 1 << 26),
    )(own, *parts)


def place_early_kernel(meta, kept0, kept1, moved0, out, zeros, sems):
    rows = kept0.shape[0]
    at = lambda place: out.at[pl.ds(place * rows, rows)]

    @pl.when(meta[0] >= 2)
    def _():
        copies = [
            pltpu.make_async_copy(source, at(place), sems.at[place])
            for source, place in ((moved0, 0), (kept0, 1), (kept1, 3))
        ]
        for copy in copies:
            copy.start()
        for copy in copies:
            copy.wait()

    @pl.when(meta[0] < 2)
    def _():
        zeros[...] = jnp.zeros_like(zeros)
        copies = [
            pltpu.make_async_copy(zeros, at(place), sems.at[place]) for place in range(BLOCKS)
        ]
        for copy in copies:
            copy.start()
        for copy in copies:
            copy.wait()


def place_early(meta, kept, moved):
    rows, width = moved.shape
    return pl.pallas_call(
        place_early_kernel,
        out_shape=pltpu.HBM((BLOCKS * rows, width), moved.dtype),
        in_specs=[smem()] + [pl.BlockSpec(memory_space=pl.ANY)] * 3,
        out_specs=hbm(),
        scratch_shapes=[pltpu.VMEM((rows, width), moved.dtype), pltpu.SemaphoreType.DMA((BLOCKS,))],
        name="place",
        **limits_of(4, 1 << 26),
    )(meta, *kept, moved)


def place_late_kernel(meta, moved1, before, out, sem):
    rows = moved1.shape[0]

    @pl.when(meta[0] >= 2)
    def _():
        copy = pltpu.make_async_copy(moved1, out.at[pl.ds(2 * rows, rows)], sem)
        copy.start()
        copy.wait()


def place_late(meta, moved, rows_out):
    return pl.pallas_call(
        place_late_kernel,
        out_shape=pltpu.HBM(rows_out.shape, rows_out.dtype),
        in_specs=[smem(), pl.BlockSpec(memory_space=pl.ANY), hbm()],
        out_specs=hbm(),
        scratch_shapes=[pltpu.SemaphoreType.DMA],
        input_output_aliases={2: 0},
        name="place",
        **limits_of(4, 1 << 26),
    )(meta, moved, rows_out)


def shards_direct(
    audio_states,
    image_states,
    audio_gain,
    image_gain,
    audio_proj,
    image_proj,
    block_rows,
    destination,
    input_gain,
    kv_weight,
):
    group = lax.axis_index("group")
    dp = lax.axis_index("dp")
    mp = lax.axis_index("mp")
    dp_count = lax.axis_size("dp")
    mp_count = lax.axis_size("mp")
    meta = jnp.stack([group, dp, mp]).astype(jnp.int32)
    rings = [[(i, (i + shift) % mp_count) for i in range(mp_count)] for shift in range(mp_count)]
    swap = [(i, (i + 1) % dp_count) for i in range(dp_count)]
    up = [(0, 2), (1, 3)]
    on_backbone = group >= 2
    full_width = input_gain.shape[0] * mp_count
    targets = 2 * dp_count
    streams = (
        (audio_states, audio_gain, audio_proj),
        (image_states, image_gain, image_proj),
    )

    messages = encode(dp_count, meta, destination, block_rows, streams)
    dealt = []
    for index in range(targets):
        c, k = index // dp_count, index % dp_count
        pairs = [(d, (2 * d + c) * dp_count + k) for d in range(dp_count)]
        pairs += [(dp_count + d, (2 * d + 1 - c) * dp_count + k) for d in range(dp_count)]
        dealt.append(lax.ppermute(messages[index], ("group", "dp"), pairs))
    gathered = []
    for stream, (_, _, proj) in enumerate(streams):
        mine = deal_index(stream, lax.rem(group, 2), dp, dp_count)
        piece = dealt[0][:, : proj.shape[0]]
        for index in range(1, targets):
            piece = jnp.where(mine == index, dealt[index][:, : proj.shape[0]], piece)
        pieces = [piece]
        for shift in range(1, mp_count):
            pieces.append(lax.ppermute(piece, "mp", rings[shift]))
        gathered.append(pieces)
    partial, others = [], []
    for stream, (_, _, proj) in enumerate(streams):
        wanted = [proj] if stream == 0 else [proj, kv_weight]
        proj, *heads_weight = fetch(wanted, (4,) * len(wanted))
        partial.append(project_rows(mp_count, meta, gathered[stream], proj, 512))
        others.append(lax.ppermute(partial[stream][1], "dp", swap))
    kept, moved, head_parts = [], [], []
    for stream in range(2):
        tokens, own, *sends = heads(
            mp_count, meta, partial[stream][0], others[stream], input_gain, heads_weight[0]
        )
        sums = []
        for shift, part in enumerate(sends, 1):
            sums.append(lax.ppermute(part, "mp", rings[shift]))
        kept.append(tokens)
        moved.append(lax.ppermute(tokens, "group", up))
        values = finish(full_width, own, sums)
        head_parts += [lax.ppermute(values, "group", up), values]
    rows_out = place_early(meta, kept, moved[0])
    rows_out = place_late(meta, moved[1], rows_out)
    heads_out = jnp.concatenate(head_parts, axis=0)
    heads_out = jnp.where(on_backbone, heads_out, jnp.zeros_like(heads_out))
    return (heads_out[None], rows_out[None])


def solution(mesh):
    if 2 * mesh.shape["dp"] != BLOCKS:
        return mapped(shards_general, mesh)
    layer = lambda *inputs: shards_direct(*inputs)
    return mapped(layer, mesh)


def mapped(shards, mesh):
    in_specs = (
        P("group", ("dp", "mp"), None),
        P("group", ("dp", "mp"), None),
        P(),
        P(),
        P("dp", "mp"),
        P("dp", "mp"),
        P(),
        P(),
        P("mp"),
        P("mp", None),
    )
    out_specs = (P("group", "dp", "mp"), P("group", "dp", "mp"))
    return jax.shard_map(shards, mesh=mesh, in_specs=in_specs, out_specs=out_specs, check_vma=False)
```

```python
import functools

import jax
import jax.numpy as jnp
from jax import lax
from jax.experimental import pallas as pl
from jax.experimental.pallas import tpu as pltpu
from jax.sharding import PartitionSpec as P


BLOCK = 128
BLOCKS = 4


EPS_LAYER = 1e-05
EPS_ROOT = 1e-06


def layer_norm(values_in, gain_vec):
    values = values_in.astype(jnp.float32)
    center = values - jnp.mean(values, axis=-1, keepdims=True)
    spread = jnp.mean(center * center, axis=-1, keepdims=True)
    return center * lax.rsqrt(spread + EPS_LAYER) * gain_vec


def route_tables(destination, dest_count):
    flat_dest = destination.reshape(-1)
    hit_table = (flat_dest[:, None] == jnp.arange(dest_count, dtype=jnp.int32)[None, :]).astype(
        jnp.int32
    )
    dest_rank = jnp.sum((jnp.cumsum(hit_table, axis=0) - 1) * hit_table, axis=1)
    per_source = hit_table.reshape(-1, BLOCKS, dest_count)
    dest_slot = jnp.sum((jnp.cumsum(per_source, axis=1) - 1) * per_source, axis=2).reshape(-1)
    return (flat_dest, dest_rank, dest_slot)


def send_index(flat_dest, dest_slot, source, targets, capacity):
    row_dest = lax.dynamic_slice_in_dim(flat_dest, source * BLOCKS, BLOCKS)
    row_slot = lax.dynamic_slice_in_dim(dest_slot, source * BLOCKS, BLOCKS)
    wanted_slot = jnp.arange(capacity, dtype=jnp.int32)
    matches = (row_dest[None, None, :] == targets[:, None, None]) & (
        row_slot[None, None, :] == wanted_slot[None, :, None]
    )
    block_ids = jnp.arange(BLOCKS, dtype=jnp.int32)
    picked_index = jnp.sum(matches.astype(jnp.int32) * block_ids[None, None, :], axis=2).reshape(-1)
    present = jnp.any(matches, axis=2).reshape(-1)
    return (picked_index, present)


def route_blocks(blocks, streams, destination, group_id, dp_index):
    dp_count = lax.axis_size("dp")
    dest_count = 2 * dp_count
    capacity = BLOCKS // 4
    flat_dest, dest_rank, dest_slot = route_tables(destination, dest_count)
    serial = jnp.arange(dest_count, dtype=jnp.int32)
    outgoing = []
    for source_blocks, stream in zip(blocks, streams):
        picked_index, present = send_index(
            flat_dest, dest_slot, stream * dp_count + dp_index, serial, capacity
        )
        present = present & (group_id == stream)
        picked = jnp.take(source_blocks, picked_index, axis=0).reshape(dest_count * capacity, -1)
        outgoing.append(jnp.where(present[:, None], picked, jnp.zeros_like(picked)))
    packed = jnp.concatenate(outgoing, axis=1)
    spare_rows = jnp.zeros_like(packed)
    moved_rows = lax.all_to_all(
        jnp.concatenate([spare_rows, packed], axis=0),
        ("group", "dp"),
        split_axis=0,
        concat_axis=0,
        tiled=True,
    )
    arrived = moved_rows[: dest_count * capacity]
    my_index = (group_id - 2) * dp_count + dp_index
    on_backbone = group_id >= 2
    block_count = flat_dest.shape[0]
    source_slot = jnp.arange(block_count, dtype=jnp.int32) // BLOCKS * capacity + dest_slot
    results = []
    offset = 0
    for source_blocks, stream in zip(blocks, streams):
        slot_width = source_blocks[0].size
        columns = arrived[:, offset : offset + slot_width]
        offset = offset + slot_width
        wanted = stream * (BLOCKS // 2) + jnp.arange(BLOCKS // 2, dtype=jnp.int32)
        matches = (flat_dest[None, :] == my_index) & (dest_rank[None, :] == wanted[:, None])
        picked_index = jnp.sum(matches.astype(jnp.int32) * source_slot[None, :], axis=1)
        taken_rows = jnp.take(columns, picked_index, axis=0)
        taken_rows = jnp.where(on_backbone, taken_rows, jnp.zeros_like(taken_rows))
        results.append(taken_rows.reshape((wanted.shape[0],) + source_blocks.shape[1:]))
    return results


def project(audio_rows, image_rows, audio_active, image_active, audio_proj, image_proj):

    def folder(row_block, active, running, shard_part):
        return lax.cond(
            active,
            lambda inner: jnp.dot(row_block, shard_part, preferred_element_type=jnp.float32),
            lambda inner: inner,
            running,
        )

    audio_start = jnp.zeros((audio_rows.shape[0], audio_proj.shape[1]), jnp.float32)
    image_start = jnp.zeros((image_rows.shape[0], image_proj.shape[1]), jnp.float32)
    audio_out = folder(
        audio_rows, audio_active, audio_start, lax.all_gather(audio_proj, "dp", axis=0, tiled=True)
    )
    image_out = folder(
        image_rows, image_active, image_start, lax.all_gather(image_proj, "dp", axis=0, tiled=True)
    )
    return (audio_out, image_out)


def shards_general(
    audio_states,
    image_states,
    audio_gain,
    image_gain,
    audio_proj,
    image_proj,
    block_rows,
    destination,
    input_gain,
    kv_weight,
):
    group_id = lax.axis_index("group")
    dp_index = lax.axis_index("dp")
    mp_index = lax.axis_index("mp")
    mp_count = lax.axis_size("mp")
    share = BLOCK // mp_count
    row_ids = mp_index * share + jnp.arange(share, dtype=jnp.int32)

    def encode(states, gain_vec, stream):
        limits = lax.dynamic_index_in_dim(block_rows[stream], dp_index, 0, keepdims=False)
        keep_rows = (row_ids[None, :] < limits[:, None]).astype(jnp.float32)
        normed = layer_norm(states[0], gain_vec).reshape(BLOCKS, share, -1)
        return (normed * keep_rows[:, :, None]).astype(jnp.bfloat16)

    audio_normed = encode(audio_states, audio_gain, 0)
    image_normed = encode(image_states, image_gain, 1)
    on_backbone = group_id >= 2
    audio_part, image_part = route_blocks(
        (audio_normed, image_normed), (0, 1), destination, group_id, dp_index
    )
    audio_full, image_full = (
        lax.all_gather(audio_part, "mp", axis=1, tiled=True),
        lax.all_gather(image_part, "mp", axis=1, tiled=True),
    )
    audio_out, image_out = project(
        audio_full.reshape(-1, audio_full.shape[2]),
        image_full.reshape(-1, image_full.shape[2]),
        on_backbone,
        on_backbone,
        audio_proj,
        image_proj,
    )
    arrived = (
        jnp.concatenate([audio_out, image_out], axis=0)
        .astype(jnp.bfloat16)
        .reshape(BLOCKS, BLOCK, -1)
    )
    token_rows = arrived.reshape(BLOCKS * BLOCK, -1)
    tokens = token_rows.astype(jnp.float32)
    squares = lax.psum(jnp.sum(tokens * tokens, axis=1), "mp")
    scaled = (tokens * input_gain).astype(jnp.bfloat16)
    partial_value = jnp.dot(scaled, kv_weight, preferred_element_type=jnp.float32)
    summed = lax.psum_scatter(partial_value, "mp", scatter_dimension=1, tiled=True)
    full_width = tokens.shape[1] * mp_count
    result = summed * lax.rsqrt(squares / full_width + EPS_ROOT)[:, None]
    return (result.astype(jnp.bfloat16)[None], token_rows[None])


MIB = 1 << 20


def smem():
    return pl.BlockSpec(memory_space=pltpu.SMEM)


def vmem():
    return pl.BlockSpec(memory_space=pltpu.VMEM)


def hbm():
    return pl.BlockSpec(memory_space=pltpu.HBM)


def in_hbm(arrays):
    return [pltpu.with_memory_space_constraint(x, pltpu.HBM) for x in arrays]


def limits_of(mib, flops=0):
    return dict(
        compiler_params=pltpu.CompilerParams(vmem_limit_bytes=mib * MIB),
        cost_estimate=pl.CostEstimate(flops=flops, transcendentals=0, bytes_accessed=0),
    )


def encode_kernel(dp_count, meta, dest, limits, *refs):
    group, dp, mp = meta[0], meta[1], meta[2]
    targets = 2 * dp_count
    inputs, messages, scratch = refs[:4], refs[4 : 4 + 2 * targets], refs[4 + 2 * targets :]
    routes, lives, *places, sems = scratch
    for stream in range(2):
        states, gain = places[2 * stream : 2 * stream + 2]
        share = states.shape[1] // BLOCKS
        half = states.shape[2] // dp_count
        outs = messages[stream * targets : (stream + 1) * targets]

        @pl.when(group == stream)
        def _():
            copies = [
                pltpu.make_async_copy(source, place, sems.at[i])
                for i, (source, place) in enumerate(
                    (
                        (dest, routes),
                        (limits, lives),
                        (inputs[2 * stream], states),
                        (inputs[2 * stream + 1], gain),
                    )
                )
            ]
            for copy in copies:
                copy.start()
            for copy in copies:
                copy.wait()
            scale = gain[...].reshape(1, -1)
            for target in range(targets):
                block = jnp.int32(0)
                for b in range(BLOCKS):
                    block = jnp.where(routes[stream, dp, b] == target, b, block)
                limit = lives[stream, dp, block]
                start = pl.multiple_of(block * share, share)
                values = states[0, pl.ds(start, share), :].astype(jnp.float32)
                center = values - jnp.mean(values, axis=-1, keepdims=True)
                spread = jnp.mean(center * center, axis=-1, keepdims=True)
                normed = center * lax.rsqrt(spread + EPS_LAYER) * scale
                row = mp * share + lax.broadcasted_iota(jnp.int32, normed.shape, 0)
                normed = jnp.where(row < limit, normed, 0.0).astype(jnp.bfloat16)
                c, home = target // dp_count, target % dp_count
                for k in range(dp_count):
                    place = 0 if home == k else 1
                    outs[c * dp_count + k][place * share : (place + 1) * share, :] = normed[
                        :, k * half : (k + 1) * half
                    ]


def encode(dp_count, meta, dest, limits, streams):
    arguments, shapes = [], []
    scratch = [pltpu.SMEM(dest.shape, jnp.int32), pltpu.SMEM(limits.shape, jnp.int32)]
    for states, gain, _ in streams:
        arguments += [states, gain]
        scratch += [pltpu.VMEM(states.shape, states.dtype), pltpu.VMEM(gain.shape, gain.dtype)]
        _, rows, width = states.shape
        shape = jax.ShapeDtypeStruct((2 * rows // BLOCKS, width // dp_count), jnp.bfloat16)
        shapes += [shape] * (2 * dp_count)
    return pl.pallas_call(
        functools.partial(encode_kernel, dp_count),
        out_shape=shapes,
        in_specs=[smem()] + [hbm()] * (2 + len(arguments)),
        out_specs=[vmem()] * len(shapes),
        scratch_shapes=scratch + [pltpu.SemaphoreType.DMA((4,))],
        name="encode",
        **limits_of(8, 1 << 28),
    )(meta, *in_hbm([dest, limits, *arguments]))


def fetch_kernel(cuts, *refs):
    count = len(cuts)
    sources, places, sems = refs[:count], refs[count : 2 * count], refs[2 * count]
    copies = []
    for source, place, pieces in zip(sources, places, cuts):
        depth = source.shape[0] // pieces
        for i in range(pieces):
            part = pl.ds(i * depth, depth)
            copies.append(
                pltpu.make_async_copy(source.at[part], place.at[part], sems.at[len(copies)])
            )
    for copy in copies:
        copy.start()
    for copy in copies:
        copy.wait()


def fetch(weights, cuts):
    return pl.pallas_call(
        functools.partial(fetch_kernel, cuts),
        out_shape=[pltpu.VMEM(x.shape, x.dtype) for x in weights],
        in_specs=[hbm()] * len(weights),
        out_specs=[vmem()] * len(weights),
        scratch_shapes=[pltpu.SemaphoreType.DMA((sum(cuts),))],
        name="fetch",
        **limits_of(12, 1 << 28),
    )(*in_hbm(weights))


def piece_source(mp, shift, mp_count):
    if mp_count == 4:
        return mp ^ shift
    return lax.rem(mp + (mp_count - shift), mp_count)


def project_half_kernel(mp_count, tile, half, meta, *refs):
    pieces, weight, result, rows = refs[:mp_count], *refs[mp_count:]
    share = pieces[0].shape[0] // 2
    for shift in range(mp_count):
        start = pl.multiple_of(piece_source(meta[2], shift, mp_count) * share, share)
        rows[pl.ds(start, share), :] = pieces[shift][half * share : (half + 1) * share, :]
    for first in range(0, weight.shape[1], tile):
        out = jnp.dot(
            rows[...], weight[:, first : first + tile], preferred_element_type=jnp.float32
        )
        result[:, first : first + tile] = out.astype(result.dtype)


def project_half(mp_count, meta, pieces, weight, tile, half):
    depth, width = weight.shape
    rows = pieces[0].shape[0] * mp_count // 2
    kind = jnp.bfloat16 if half else jnp.float32
    return pl.pallas_call(
        functools.partial(project_half_kernel, mp_count, tile, half),
        out_shape=jax.ShapeDtypeStruct((rows, width), kind),
        in_specs=[smem()] + [vmem()] * (mp_count + 1),
        out_specs=vmem(),
        scratch_shapes=[pltpu.VMEM((rows, depth), jnp.bfloat16)],
        name="project",
        **limits_of(12, 2 * rows * depth * width),
    )(meta, *pieces, weight)


def project_kernel(mp_count, tile, meta, *refs):
    pieces, weight, keep, send, rows = refs[:mp_count], *refs[mp_count:]
    share = pieces[0].shape[0] // 2
    block = share * mp_count
    for shift in range(mp_count):
        source = piece_source(meta[2], shift, mp_count)
        start = pl.multiple_of(source * share, share)
        rows[pl.ds(start, share), :] = pieces[shift][:share, :]
        rows[pl.ds(block + start, share), :] = pieces[shift][share:, :]
    for first in range(0, weight.shape[1], tile):
        out = jnp.dot(
            rows[...], weight[:, first : first + tile], preferred_element_type=jnp.float32
        )
        keep[:, first : first + tile] = out[:block]
        send[:, first : first + tile] = out[block:].astype(jnp.bfloat16)


def project_rows(mp_count, meta, pieces, weight, tile):
    depth, width = weight.shape
    rows = pieces[0].shape[0] * mp_count
    return pl.pallas_call(
        functools.partial(project_kernel, mp_count, tile),
        out_shape=[
            jax.ShapeDtypeStruct((rows // 2, width), jnp.float32),
            jax.ShapeDtypeStruct((rows // 2, width), jnp.bfloat16),
        ],
        in_specs=[smem()] + [vmem()] * (mp_count + 1),
        out_specs=[vmem()] * 2,
        scratch_shapes=[pltpu.VMEM((rows, depth), jnp.bfloat16)],
        name="project",
        **limits_of(12, 2 * rows * depth * width),
    )(meta, *pieces, weight)


def heads_kernel(mp_count, meta, keep, other, gain, weight, tokens, own, *rest):
    sends, scaled = rest[:-1], rest[-1]
    rows, tile = own.shape[0] - 8, own.shape[1]
    rounded = (keep[...] + other[...].astype(jnp.float32)).astype(jnp.bfloat16)
    tokens[...] = rounded
    values = rounded.astype(jnp.float32)
    scaled[...] = (values * gain[...].reshape(1, -1)).astype(jnp.bfloat16)
    total = jnp.sum(values * values, axis=1, keepdims=True)
    turned = jnp.transpose(jnp.broadcast_to(total, (rows, 128)))[:8]
    high = turned.astype(jnp.bfloat16).astype(jnp.float32)
    line = lax.broadcasted_iota(jnp.int32, turned.shape, 0)
    packed = jnp.where(line == 0, high, jnp.where(line == 1, turned - high, 0.0))
    packed = jnp.concatenate([packed] + [jnp.zeros((8, tile - rows), jnp.float32)], axis=1)
    for shift in list(range(1, mp_count)) + [0]:
        chunk = lax.rem(meta[2] + shift, mp_count)
        columns = pl.ds(pl.multiple_of(chunk * tile, tile), tile)
        out = jnp.dot(scaled[...], weight[:, columns], preferred_element_type=jnp.float32)
        if shift:
            block = jnp.concatenate([out, packed], axis=0)
            sends[shift - 1][...] = block.astype(jnp.bfloat16)
        else:
            own[:rows, :] = out
            own[rows:, :] = packed


def heads(mp_count, meta, keep, other, gain, weight):
    rows, width = keep.shape
    tile = weight.shape[1] // mp_count
    return pl.pallas_call(
        functools.partial(heads_kernel, mp_count),
        in_specs=[smem()] + [vmem()] * 4,
        out_specs=[vmem()] * (1 + mp_count),
        scratch_shapes=[pltpu.VMEM((rows, width), jnp.bfloat16)],
        out_shape=[
            jax.ShapeDtypeStruct((rows, width), jnp.bfloat16),
            jax.ShapeDtypeStruct((rows + 8, tile), jnp.float32),
        ]
        + [jax.ShapeDtypeStruct((rows + 8, tile), jnp.bfloat16)] * (mp_count - 1),
        name="heads",
        **limits_of(14, 2 * rows * width * weight.shape[1]),
    )(meta, keep, other, gain, weight)


def finish_kernel(full_width, own, *refs):
    parts, result = refs[:-1], refs[-1]
    rows = result.shape[0]
    total = own[...]
    for part in parts:
        total = total + part[...].astype(jnp.float32)
    square = total[rows : rows + 1, :rows] + total[rows + 1 : rows + 2, :rows]
    scale = lax.rsqrt(square / full_width + EPS_ROOT)
    column = jnp.transpose(jnp.broadcast_to(scale, (128, rows)))[:, :1]
    result[...] = (total[:rows] * column).astype(jnp.bfloat16)


def finish(full_width, own, parts):
    rows, tile = own.shape
    return pl.pallas_call(
        functools.partial(finish_kernel, full_width),
        out_shape=jax.ShapeDtypeStruct((rows - 8, tile), jnp.bfloat16),
        in_specs=[vmem()] * (1 + len(parts)),
        out_specs=vmem(),
        name="finish",
        **limits_of(4, 1 << 26),
    )(own, *parts)


def place_early_kernel(meta, kept0, kept1, moved0, out, zeros, sems):
    rows = kept0.shape[0]
    at = lambda place: out.at[pl.ds(place * rows, rows)]

    @pl.when(meta[0] >= 2)
    def _():
        copies = [
            pltpu.make_async_copy(source, at(place), sems.at[place])
            for source, place in ((moved0, 0), (kept0, 1), (kept1, 3))
        ]
        for copy in copies:
            copy.start()
        for copy in copies:
            copy.wait()

    @pl.when(meta[0] < 2)
    def _():
        zeros[...] = jnp.zeros_like(zeros)
        copies = [
            pltpu.make_async_copy(zeros, at(place), sems.at[place]) for place in range(BLOCKS)
        ]
        for copy in copies:
            copy.start()
        for copy in copies:
            copy.wait()


def place_early(meta, kept, moved):
    rows, width = moved.shape
    return pl.pallas_call(
        place_early_kernel,
        out_shape=pltpu.HBM((BLOCKS * rows, width), moved.dtype),
        in_specs=[smem()] + [pl.BlockSpec(memory_space=pl.ANY)] * 3,
        out_specs=hbm(),
        scratch_shapes=[pltpu.VMEM((rows, width), moved.dtype), pltpu.SemaphoreType.DMA((BLOCKS,))],
        name="place",
        **limits_of(4, 1 << 26),
    )(meta, *kept, moved)


def place_late_kernel(meta, moved1, before, out, sem):
    rows = moved1.shape[0]

    @pl.when(meta[0] >= 2)
    def _():
        copy = pltpu.make_async_copy(moved1, out.at[pl.ds(2 * rows, rows)], sem)
        copy.start()
        copy.wait()


def place_late(meta, moved, rows_out):
    return pl.pallas_call(
        place_late_kernel,
        out_shape=pltpu.HBM(rows_out.shape, rows_out.dtype),
        in_specs=[smem(), pl.BlockSpec(memory_space=pl.ANY), hbm()],
        out_specs=hbm(),
        scratch_shapes=[pltpu.SemaphoreType.DMA],
        input_output_aliases={2: 0},
        name="place",
        **limits_of(4, 1 << 26),
    )(meta, moved, rows_out)


def shards_direct(
    audio_states,
    image_states,
    audio_gain,
    image_gain,
    audio_proj,
    image_proj,
    block_rows,
    destination,
    input_gain,
    kv_weight,
):
    group = lax.axis_index("group")
    dp = lax.axis_index("dp")
    mp = lax.axis_index("mp")
    dp_count = lax.axis_size("dp")
    mp_count = lax.axis_size("mp")
    meta = jnp.stack([group, dp, mp]).astype(jnp.int32)
    rings = [[(i, (i + shift) % mp_count) for i in range(mp_count)] for shift in range(mp_count)]
    spreads = rings
    if mp_count == 4:
        spreads = [[(i, i ^ step) for i in range(mp_count)] for step in (0, 1, 2, 1)]
    swap = [(i, (i + 1) % dp_count) for i in range(dp_count)]
    up = [(0, 2), (1, 3)]
    on_backbone = group >= 2
    full_width = input_gain.shape[0] * mp_count
    targets = 2 * dp_count
    streams = (
        (audio_states, audio_gain, audio_proj),
        (image_states, image_gain, image_proj),
    )

    messages = encode(dp_count, meta, destination, block_rows, streams)
    mine = lax.rem(group, 2) * dp_count + dp
    gathered = []
    for stream in range(2):
        piece = None
        for index in range(targets):
            c, k = index // dp_count, index % dp_count
            pairs = [(stream * dp_count + d, (2 * d + c) * dp_count + k) for d in range(dp_count)]
            moved = lax.ppermute(messages[stream * targets + index], ("group", "dp"), pairs)
            piece = moved if piece is None else jnp.where(mine == index, moved, piece)
        pieces = [piece]
        for shift in range(1, mp_count):
            sent = pieces[2] if mp_count == 4 and shift == 3 else piece
            pieces.append(lax.ppermute(sent, "mp", spreads[shift]))
        gathered.append(pieces)
    partial, others = [], []
    for stream, (_, _, proj) in enumerate(streams):
        (proj,) = fetch([proj], (4,))
        if stream == 0:
            keep, send = project_rows(mp_count, meta, gathered[stream], proj, 512)
        else:
            send = project_half(mp_count, meta, gathered[stream], proj, 512, 1)
            keep = project_half(mp_count, meta, gathered[stream], proj, 512, 0)
        partial.append((keep, send))
        others.append(lax.ppermute(send, "dp", swap))
    (heads_weight,) = fetch([kv_weight], (8,))
    kept, moved, head_parts = [], [], []
    for stream in range(2):
        tokens, own, *sends = heads(
            mp_count, meta, partial[stream][0], others[stream], input_gain, heads_weight
        )
        sums = []
        for shift, part in enumerate(sends, 1):
            sums.append(lax.ppermute(part, "mp", rings[shift]))
        kept.append(tokens)
        moved.append(lax.ppermute(tokens, "group", up))
        values = finish(full_width, own, sums)
        head_parts += [lax.ppermute(values, "group", up), values]
    rows_out = place_early(meta, kept, moved[0])
    rows_out = place_late(meta, moved[1], rows_out)
    heads_out = jnp.concatenate(head_parts, axis=0)
    heads_out = jnp.where(on_backbone, heads_out, jnp.zeros_like(heads_out))
    return (heads_out[None], rows_out[None])


def solution(mesh):
    if 2 * mesh.shape["dp"] != BLOCKS:
        return mapped(shards_general, mesh)
    layer = lambda *inputs: shards_direct(*inputs)
    return mapped(layer, mesh)


def mapped(shards, mesh):
    in_specs = (
        P("group", ("dp", "mp"), None),
        P("group", ("dp", "mp"), None),
        P(),
        P(),
        P("dp", "mp"),
        P("dp", "mp"),
        P(),
        P(),
        P("mp"),
        P("mp", None),
    )
    out_specs = (P("group", "dp", "mp"), P("group", "dp", "mp"))
    return jax.shard_map(shards, mesh=mesh, in_specs=in_specs, out_specs=out_specs, check_vma=False)
```

```python
import functools

import jax
import jax.numpy as jnp
from jax import lax
from jax.experimental import pallas as pl
from jax.experimental.pallas import tpu as pltpu
from jax.sharding import PartitionSpec as P


BLOCK = 128
BLOCKS = 4


EPS_LAYER = 1e-05
EPS_ROOT = 1e-06


def layer_norm(values_in, gain_vec):
    values = values_in.astype(jnp.float32)
    center = values - jnp.mean(values, axis=-1, keepdims=True)
    spread = jnp.mean(center * center, axis=-1, keepdims=True)
    return center * lax.rsqrt(spread + EPS_LAYER) * gain_vec


def route_tables(destination, dest_count):
    flat_dest = destination.reshape(-1)
    hit_table = (flat_dest[:, None] == jnp.arange(dest_count, dtype=jnp.int32)[None, :]).astype(
        jnp.int32
    )
    dest_rank = jnp.sum((jnp.cumsum(hit_table, axis=0) - 1) * hit_table, axis=1)
    per_source = hit_table.reshape(-1, BLOCKS, dest_count)
    dest_slot = jnp.sum((jnp.cumsum(per_source, axis=1) - 1) * per_source, axis=2).reshape(-1)
    return (flat_dest, dest_rank, dest_slot)


def send_index(flat_dest, dest_slot, source, targets, capacity):
    row_dest = lax.dynamic_slice_in_dim(flat_dest, source * BLOCKS, BLOCKS)
    row_slot = lax.dynamic_slice_in_dim(dest_slot, source * BLOCKS, BLOCKS)
    wanted_slot = jnp.arange(capacity, dtype=jnp.int32)
    matches = (row_dest[None, None, :] == targets[:, None, None]) & (
        row_slot[None, None, :] == wanted_slot[None, :, None]
    )
    block_ids = jnp.arange(BLOCKS, dtype=jnp.int32)
    picked_index = jnp.sum(matches.astype(jnp.int32) * block_ids[None, None, :], axis=2).reshape(-1)
    present = jnp.any(matches, axis=2).reshape(-1)
    return (picked_index, present)


def route_blocks(blocks, streams, destination, group_id, dp_index):
    dp_count = lax.axis_size("dp")
    dest_count = 2 * dp_count
    capacity = BLOCKS // 4
    flat_dest, dest_rank, dest_slot = route_tables(destination, dest_count)
    serial = jnp.arange(dest_count, dtype=jnp.int32)
    outgoing = []
    for source_blocks, stream in zip(blocks, streams):
        picked_index, present = send_index(
            flat_dest, dest_slot, stream * dp_count + dp_index, serial, capacity
        )
        present = present & (group_id == stream)
        picked = jnp.take(source_blocks, picked_index, axis=0).reshape(dest_count * capacity, -1)
        outgoing.append(jnp.where(present[:, None], picked, jnp.zeros_like(picked)))
    packed = jnp.concatenate(outgoing, axis=1)
    spare_rows = jnp.zeros_like(packed)
    moved_rows = lax.all_to_all(
        jnp.concatenate([spare_rows, packed], axis=0),
        ("group", "dp"),
        split_axis=0,
        concat_axis=0,
        tiled=True,
    )
    arrived = moved_rows[: dest_count * capacity]
    my_index = (group_id - 2) * dp_count + dp_index
    on_backbone = group_id >= 2
    block_count = flat_dest.shape[0]
    source_slot = jnp.arange(block_count, dtype=jnp.int32) // BLOCKS * capacity + dest_slot
    results = []
    offset = 0
    for source_blocks, stream in zip(blocks, streams):
        slot_width = source_blocks[0].size
        columns = arrived[:, offset : offset + slot_width]
        offset = offset + slot_width
        wanted = stream * (BLOCKS // 2) + jnp.arange(BLOCKS // 2, dtype=jnp.int32)
        matches = (flat_dest[None, :] == my_index) & (dest_rank[None, :] == wanted[:, None])
        picked_index = jnp.sum(matches.astype(jnp.int32) * source_slot[None, :], axis=1)
        taken_rows = jnp.take(columns, picked_index, axis=0)
        taken_rows = jnp.where(on_backbone, taken_rows, jnp.zeros_like(taken_rows))
        results.append(taken_rows.reshape((wanted.shape[0],) + source_blocks.shape[1:]))
    return results


def project(audio_rows, image_rows, audio_active, image_active, audio_proj, image_proj):

    def folder(row_block, active, running, shard_part):
        return lax.cond(
            active,
            lambda inner: jnp.dot(row_block, shard_part, preferred_element_type=jnp.float32),
            lambda inner: inner,
            running,
        )

    audio_start = jnp.zeros((audio_rows.shape[0], audio_proj.shape[1]), jnp.float32)
    image_start = jnp.zeros((image_rows.shape[0], image_proj.shape[1]), jnp.float32)
    audio_out = folder(
        audio_rows, audio_active, audio_start, lax.all_gather(audio_proj, "dp", axis=0, tiled=True)
    )
    image_out = folder(
        image_rows, image_active, image_start, lax.all_gather(image_proj, "dp", axis=0, tiled=True)
    )
    return (audio_out, image_out)


def shards_general(
    audio_states,
    image_states,
    audio_gain,
    image_gain,
    audio_proj,
    image_proj,
    block_rows,
    destination,
    input_gain,
    kv_weight,
):
    group_id = lax.axis_index("group")
    dp_index = lax.axis_index("dp")
    mp_index = lax.axis_index("mp")
    mp_count = lax.axis_size("mp")
    share = BLOCK // mp_count
    row_ids = mp_index * share + jnp.arange(share, dtype=jnp.int32)

    def encode(states, gain_vec, stream):
        limits = lax.dynamic_index_in_dim(block_rows[stream], dp_index, 0, keepdims=False)
        keep_rows = (row_ids[None, :] < limits[:, None]).astype(jnp.float32)
        normed = layer_norm(states[0], gain_vec).reshape(BLOCKS, share, -1)
        return (normed * keep_rows[:, :, None]).astype(jnp.bfloat16)

    audio_normed = encode(audio_states, audio_gain, 0)
    image_normed = encode(image_states, image_gain, 1)
    on_backbone = group_id >= 2
    audio_part, image_part = route_blocks(
        (audio_normed, image_normed), (0, 1), destination, group_id, dp_index
    )
    audio_full, image_full = (
        lax.all_gather(audio_part, "mp", axis=1, tiled=True),
        lax.all_gather(image_part, "mp", axis=1, tiled=True),
    )
    audio_out, image_out = project(
        audio_full.reshape(-1, audio_full.shape[2]),
        image_full.reshape(-1, image_full.shape[2]),
        on_backbone,
        on_backbone,
        audio_proj,
        image_proj,
    )
    arrived = (
        jnp.concatenate([audio_out, image_out], axis=0)
        .astype(jnp.bfloat16)
        .reshape(BLOCKS, BLOCK, -1)
    )
    token_rows = arrived.reshape(BLOCKS * BLOCK, -1)
    tokens = token_rows.astype(jnp.float32)
    squares = lax.psum(jnp.sum(tokens * tokens, axis=1), "mp")
    scaled = (tokens * input_gain).astype(jnp.bfloat16)
    partial_value = jnp.dot(scaled, kv_weight, preferred_element_type=jnp.float32)
    summed = lax.psum_scatter(partial_value, "mp", scatter_dimension=1, tiled=True)
    full_width = tokens.shape[1] * mp_count
    result = summed * lax.rsqrt(squares / full_width + EPS_ROOT)[:, None]
    return (result.astype(jnp.bfloat16)[None], token_rows[None])


MIB = 1 << 20


class Place:
    def __getitem__(self, axis):
        return lax.axis_index(("group", "dp", "mp")[axis])


def vmem():
    return pl.BlockSpec(memory_space=pltpu.VMEM)


def hbm():
    return pl.BlockSpec(memory_space=pltpu.HBM)


def in_hbm(arrays):
    return [pltpu.with_memory_space_constraint(x, pltpu.HBM) for x in arrays]


def limits_of(mib, flops=0):
    return dict(
        compiler_params=pltpu.CompilerParams(vmem_limit_bytes=mib * MIB),
        cost_estimate=pl.CostEstimate(flops=flops, transcendentals=0, bytes_accessed=0),
    )


def encode_kernel(dp_count, dest, limits, *refs):
    meta = Place()
    group, dp, mp = meta[0], meta[1], meta[2]
    targets = 2 * dp_count
    inputs, messages, scratch = refs[:4], refs[4 : 4 + 2 * targets], refs[4 + 2 * targets :]
    routes, lives, *places, sems = scratch
    for stream in range(2):
        states, gain = places[2 * stream : 2 * stream + 2]
        share = states.shape[1] // BLOCKS
        half = states.shape[2] // dp_count
        outs = messages[stream * targets : (stream + 1) * targets]

        @pl.when(group == stream)
        def _():
            copies = [
                pltpu.make_async_copy(source, place, sems.at[i])
                for i, (source, place) in enumerate(
                    (
                        (dest, routes),
                        (limits, lives),
                        (inputs[2 * stream + 1], gain),
                    )
                )
            ]
            for b in range(BLOCKS):
                part = (0, pl.ds(b * share, share))
                copies.append(
                    pltpu.make_async_copy(
                        inputs[2 * stream].at[part], states.at[part], sems.at[len(copies)]
                    )
                )
            for copy in copies:
                copy.start()
            for copy in copies:
                copy.wait()
            scale = gain[...].reshape(1, -1)
            for target in range(targets):
                block = jnp.int32(0)
                for b in range(BLOCKS):
                    block = jnp.where(routes[stream, dp, b] == target, b, block)
                limit = lives[stream, dp, block]
                start = pl.multiple_of(block * share, share)
                values = states[0, pl.ds(start, share), :].astype(jnp.float32)
                center = values - jnp.mean(values, axis=-1, keepdims=True)
                spread = jnp.mean(center * center, axis=-1, keepdims=True)
                normed = center * lax.rsqrt(spread + EPS_LAYER) * scale
                row = mp * share + lax.broadcasted_iota(jnp.int32, normed.shape, 0)
                normed = jnp.where(row < limit, normed, 0.0).astype(jnp.bfloat16)
                c, home = target // dp_count, target % dp_count
                for k in range(dp_count):
                    place = 0 if home == k else 1
                    outs[c * dp_count + k][place * share : (place + 1) * share, :] = normed[
                        :, k * half : (k + 1) * half
                    ]


def encode(dp_count, dest, limits, streams):
    arguments, shapes = [], []
    scratch = [pltpu.SMEM(dest.shape, jnp.int32), pltpu.SMEM(limits.shape, jnp.int32)]
    for states, gain, _ in streams:
        arguments += [states, gain]
        scratch += [pltpu.VMEM(states.shape, states.dtype), pltpu.VMEM(gain.shape, gain.dtype)]
        _, rows, width = states.shape
        shape = jax.ShapeDtypeStruct((2 * rows // BLOCKS, width // dp_count), jnp.bfloat16)
        shapes += [shape] * (2 * dp_count)
    return pl.pallas_call(
        functools.partial(encode_kernel, dp_count),
        out_shape=shapes,
        in_specs=[hbm()] * (2 + len(arguments)),
        out_specs=[vmem()] * len(shapes),
        scratch_shapes=scratch + [pltpu.SemaphoreType.DMA((3 + BLOCKS,))],
        name="encode",
        **limits_of(8, 1 << 28),
    )(*in_hbm([dest, limits, *arguments]))


def fetch_kernel(cuts, *refs):
    count = len(cuts)
    sources, places, sems = refs[:count], refs[count : 2 * count], refs[2 * count]
    copies = []
    for source, place, pieces in zip(sources, places, cuts):
        depth = source.shape[0] // pieces
        for i in range(pieces):
            part = pl.ds(i * depth, depth)
            copies.append(
                pltpu.make_async_copy(source.at[part], place.at[part], sems.at[len(copies)])
            )
    for copy in copies:
        copy.start()
    for copy in copies:
        copy.wait()


def fetch(weights, cuts):
    return pl.pallas_call(
        functools.partial(fetch_kernel, cuts),
        out_shape=[pltpu.VMEM(x.shape, x.dtype) for x in weights],
        in_specs=[hbm()] * len(weights),
        out_specs=[vmem()] * len(weights),
        scratch_shapes=[pltpu.SemaphoreType.DMA((sum(cuts),))],
        name="fetch",
        **limits_of(12, 1 << 28),
    )(*in_hbm(weights))


def piece_source(mp, shift, mp_count):
    if mp_count == 4:
        return mp ^ shift
    return lax.rem(mp + (mp_count - shift), mp_count)


def project_half_kernel(mp_count, tile, half, *refs):
    meta = Place()
    pieces, weight, result, rows = refs[:mp_count], *refs[mp_count:]
    share = pieces[0].shape[0] // 2
    for shift in range(mp_count):
        start = pl.multiple_of(piece_source(meta[2], shift, mp_count) * share, share)
        rows[pl.ds(start, share), :] = pieces[shift][half * share : (half + 1) * share, :]
    for first in range(0, weight.shape[1], tile):
        out = jnp.dot(
            rows[...], weight[:, first : first + tile], preferred_element_type=jnp.float32
        )
        result[:, first : first + tile] = out.astype(result.dtype)


def project_half(mp_count, pieces, weight, tile, half):
    depth, width = weight.shape
    rows = pieces[0].shape[0] * mp_count // 2
    kind = jnp.bfloat16 if half else jnp.float32
    return pl.pallas_call(
        functools.partial(project_half_kernel, mp_count, tile, half),
        out_shape=jax.ShapeDtypeStruct((rows, width), kind),
        in_specs=[vmem()] * (mp_count + 1),
        out_specs=vmem(),
        scratch_shapes=[pltpu.VMEM((rows, depth), jnp.bfloat16)],
        name="project",
        **limits_of(12, 2 * rows * depth * width),
    )(*pieces, weight)


def project_kernel(mp_count, tile, *refs):
    meta = Place()
    pieces, weight, keep, send, rows = refs[:mp_count], *refs[mp_count:]
    share = pieces[0].shape[0] // 2
    block = share * mp_count
    for shift in range(mp_count):
        source = piece_source(meta[2], shift, mp_count)
        start = pl.multiple_of(source * share, share)
        rows[pl.ds(start, share), :] = pieces[shift][:share, :]
        rows[pl.ds(block + start, share), :] = pieces[shift][share:, :]
    for first in range(0, weight.shape[1], tile):
        out = jnp.dot(
            rows[...], weight[:, first : first + tile], preferred_element_type=jnp.float32
        )
        keep[:, first : first + tile] = out[:block]
        send[:, first : first + tile] = out[block:].astype(jnp.bfloat16)


def project_rows(mp_count, pieces, weight, tile):
    depth, width = weight.shape
    rows = pieces[0].shape[0] * mp_count
    return pl.pallas_call(
        functools.partial(project_kernel, mp_count, tile),
        out_shape=[
            jax.ShapeDtypeStruct((rows // 2, width), jnp.float32),
            jax.ShapeDtypeStruct((rows // 2, width), jnp.bfloat16),
        ],
        in_specs=[vmem()] * (mp_count + 1),
        out_specs=[vmem()] * 2,
        scratch_shapes=[pltpu.VMEM((rows, depth), jnp.bfloat16)],
        name="project",
        **limits_of(12, 2 * rows * depth * width),
    )(*pieces, weight)


def heads_kernel(mp_count, keep, other, gain, weight, tokens, own, *rest):
    meta = Place()
    sends, scaled = rest[:-1], rest[-1]
    rows, tile = own.shape[0] - 8, own.shape[1]
    rounded = (keep[...] + other[...].astype(jnp.float32)).astype(jnp.bfloat16)
    tokens[...] = rounded
    values = rounded.astype(jnp.float32)
    scaled[...] = (values * gain[...].reshape(1, -1)).astype(jnp.bfloat16)
    total = jnp.sum(values * values, axis=1, keepdims=True)
    turned = jnp.transpose(jnp.broadcast_to(total, (rows, 128)))[:8]
    high = turned.astype(jnp.bfloat16).astype(jnp.float32)
    line = lax.broadcasted_iota(jnp.int32, turned.shape, 0)
    packed = jnp.where(line == 0, high, jnp.where(line == 1, turned - high, 0.0))
    packed = jnp.concatenate([packed] + [jnp.zeros((8, tile - rows), jnp.float32)], axis=1)
    for shift in list(range(1, mp_count)) + [0]:
        chunk = lax.rem(meta[2] + shift, mp_count)
        columns = pl.ds(pl.multiple_of(chunk * tile, tile), tile)
        out = jnp.dot(scaled[...], weight[:, columns], preferred_element_type=jnp.float32)
        if shift:
            block = jnp.concatenate([out, packed], axis=0)
            sends[shift - 1][...] = block.astype(jnp.bfloat16)
        else:
            own[:rows, :] = out
            own[rows:, :] = packed


def heads(mp_count, keep, other, gain, weight):
    rows, width = keep.shape
    tile = weight.shape[1] // mp_count
    return pl.pallas_call(
        functools.partial(heads_kernel, mp_count),
        in_specs=[vmem()] * 4,
        out_specs=[vmem()] * (1 + mp_count),
        scratch_shapes=[pltpu.VMEM((rows, width), jnp.bfloat16)],
        out_shape=[
            jax.ShapeDtypeStruct((rows, width), jnp.bfloat16),
            jax.ShapeDtypeStruct((rows + 8, tile), jnp.float32),
        ]
        + [jax.ShapeDtypeStruct((rows + 8, tile), jnp.bfloat16)] * (mp_count - 1),
        name="heads",
        **limits_of(14, 2 * rows * width * weight.shape[1]),
    )(keep, other, gain, weight)


def finish_kernel(full_width, own, *refs):
    parts, result = refs[:-1], refs[-1]
    rows = result.shape[0]
    total = own[...]
    for part in parts:
        total = total + part[...].astype(jnp.float32)
    square = total[rows : rows + 1, :rows] + total[rows + 1 : rows + 2, :rows]
    scale = lax.rsqrt(square / full_width + EPS_ROOT)
    column = jnp.transpose(jnp.broadcast_to(scale, (128, rows)))[:, :1]
    result[...] = (total[:rows] * column).astype(jnp.bfloat16)


def finish(full_width, own, parts):
    rows, tile = own.shape
    return pl.pallas_call(
        functools.partial(finish_kernel, full_width),
        out_shape=jax.ShapeDtypeStruct((rows - 8, tile), jnp.bfloat16),
        in_specs=[vmem()] * (1 + len(parts)),
        out_specs=vmem(),
        name="finish",
        **limits_of(4, 1 << 26),
    )(own, *parts)


def place_early_kernel(kept0, kept1, moved0, out, zeros, sems):
    meta = Place()
    rows = kept0.shape[0]
    at = lambda place: out.at[pl.ds(place * rows, rows)]

    @pl.when(meta[0] >= 2)
    def _():
        copies = [
            pltpu.make_async_copy(source, at(place), sems.at[place])
            for source, place in ((moved0, 0), (kept0, 1), (kept1, 3))
        ]
        for copy in copies:
            copy.start()
        for copy in copies:
            copy.wait()

    @pl.when(meta[0] < 2)
    def _():
        zeros[...] = jnp.zeros_like(zeros)
        copies = [
            pltpu.make_async_copy(zeros, at(place), sems.at[place]) for place in range(BLOCKS)
        ]
        for copy in copies:
            copy.start()
        for copy in copies:
            copy.wait()


def place_early(kept, moved):
    rows, width = moved.shape
    return pl.pallas_call(
        place_early_kernel,
        out_shape=pltpu.HBM((BLOCKS * rows, width), moved.dtype),
        in_specs=[pl.BlockSpec(memory_space=pl.ANY)] * 3,
        out_specs=hbm(),
        scratch_shapes=[pltpu.VMEM((rows, width), moved.dtype), pltpu.SemaphoreType.DMA((BLOCKS,))],
        name="place",
        **limits_of(4, 1 << 26),
    )(*kept, moved)


def place_late_kernel(moved1, before, out, sem):
    meta = Place()
    rows = moved1.shape[0]

    @pl.when(meta[0] >= 2)
    def _():
        copy = pltpu.make_async_copy(moved1, out.at[pl.ds(2 * rows, rows)], sem)
        copy.start()
        copy.wait()


def place_late(moved, rows_out):
    return pl.pallas_call(
        place_late_kernel,
        out_shape=pltpu.HBM(rows_out.shape, rows_out.dtype),
        in_specs=[pl.BlockSpec(memory_space=pl.ANY), hbm()],
        out_specs=hbm(),
        scratch_shapes=[pltpu.SemaphoreType.DMA],
        input_output_aliases={1: 0},
        name="place",
        **limits_of(4, 1 << 26),
    )(moved, rows_out)


def shards_direct(
    audio_states,
    image_states,
    audio_gain,
    image_gain,
    audio_proj,
    image_proj,
    block_rows,
    destination,
    input_gain,
    kv_weight,
):
    group = lax.axis_index("group")
    dp = lax.axis_index("dp")
    dp_count = lax.axis_size("dp")
    mp_count = lax.axis_size("mp")
    rings = [[(i, (i + shift) % mp_count) for i in range(mp_count)] for shift in range(mp_count)]
    spreads = rings
    if mp_count == 4:
        spreads = [[(i, i ^ step) for i in range(mp_count)] for step in (0, 1, 2, 1)]
    swap = [(i, (i + 1) % dp_count) for i in range(dp_count)]
    up = [(0, 2), (1, 3)]
    on_backbone = group >= 2
    full_width = input_gain.shape[0] * mp_count
    targets = 2 * dp_count
    streams = (
        (audio_states, audio_gain, audio_proj),
        (image_states, image_gain, image_proj),
    )

    messages = encode(dp_count, destination, block_rows, streams)
    mine = lax.rem(group, 2) * dp_count + dp
    gathered = []
    for stream in range(2):
        piece = None
        for index in range(targets):
            c, k = index // dp_count, index % dp_count
            pairs = [(stream * dp_count + d, (2 * d + c) * dp_count + k) for d in range(dp_count)]
            moved = lax.ppermute(messages[stream * targets + index], ("group", "dp"), pairs)
            piece = moved if piece is None else jnp.where(mine == index, moved, piece)
        pieces = [piece]
        for shift in range(1, mp_count):
            sent = pieces[2] if mp_count == 4 and shift == 3 else piece
            pieces.append(lax.ppermute(sent, "mp", spreads[shift]))
        gathered.append(pieces)
    partial, others = [], []
    for stream, (_, _, proj) in enumerate(streams):
        (proj,) = fetch([proj], (4,))
        if stream == 0:
            keep, send = project_rows(mp_count, gathered[stream], proj, 512)
        else:
            send = project_half(mp_count, gathered[stream], proj, 512, 1)
            keep = project_half(mp_count, gathered[stream], proj, 512, 0)
        partial.append((keep, send))
        others.append(lax.ppermute(send, "dp", swap))
    (heads_weight,) = fetch([kv_weight], (8,))
    kept, moved, head_parts = [], [], []
    for stream in range(2):
        tokens, own, *sends = heads(
            mp_count, partial[stream][0], others[stream], input_gain, heads_weight
        )
        sums = []
        for shift, part in enumerate(sends, 1):
            sums.append(lax.ppermute(part, "mp", rings[shift]))
        kept.append(tokens)
        moved.append(lax.ppermute(tokens, "group", up))
        values = finish(full_width, own, sums)
        head_parts += [lax.ppermute(values, "group", up), values]
    rows_out = place_early(kept, moved[0])
    rows_out = place_late(moved[1], rows_out)
    heads_out = jnp.concatenate(head_parts, axis=0)
    heads_out = jnp.where(on_backbone, heads_out, jnp.zeros_like(heads_out))
    return (heads_out[None], rows_out[None])


def solution(mesh):
    if 2 * mesh.shape["dp"] != BLOCKS:
        return mapped(shards_general, mesh)
    layer = lambda *inputs: shards_direct(*inputs)
    return mapped(layer, mesh)


def mapped(shards, mesh):
    in_specs = (
        P("group", ("dp", "mp"), None),
        P("group", ("dp", "mp"), None),
        P(),
        P(),
        P("dp", "mp"),
        P("dp", "mp"),
        P(),
        P(),
        P("mp"),
        P("mp", None),
    )
    out_specs = (P("group", "dp", "mp"), P("group", "dp", "mp"))
    return jax.shard_map(shards, mesh=mesh, in_specs=in_specs, out_specs=out_specs, check_vma=False)
```

```python
import functools

import jax
import jax.numpy as jnp
from jax import lax
from jax.experimental import pallas as pl
from jax.experimental.pallas import tpu as pltpu
from jax.sharding import PartitionSpec as P


BLOCK = 128
BLOCKS = 4


EPS_LAYER = 1e-05
EPS_ROOT = 1e-06


def layer_norm(values_in, gain_vec):
    values = values_in.astype(jnp.float32)
    center = values - jnp.mean(values, axis=-1, keepdims=True)
    spread = jnp.mean(center * center, axis=-1, keepdims=True)
    return center * lax.rsqrt(spread + EPS_LAYER) * gain_vec


def route_tables(destination, dest_count):
    flat_dest = destination.reshape(-1)
    hit_table = (flat_dest[:, None] == jnp.arange(dest_count, dtype=jnp.int32)[None, :]).astype(
        jnp.int32
    )
    dest_rank = jnp.sum((jnp.cumsum(hit_table, axis=0) - 1) * hit_table, axis=1)
    per_source = hit_table.reshape(-1, BLOCKS, dest_count)
    dest_slot = jnp.sum((jnp.cumsum(per_source, axis=1) - 1) * per_source, axis=2).reshape(-1)
    return (flat_dest, dest_rank, dest_slot)


def send_index(flat_dest, dest_slot, source, targets, capacity):
    row_dest = lax.dynamic_slice_in_dim(flat_dest, source * BLOCKS, BLOCKS)
    row_slot = lax.dynamic_slice_in_dim(dest_slot, source * BLOCKS, BLOCKS)
    wanted_slot = jnp.arange(capacity, dtype=jnp.int32)
    matches = (row_dest[None, None, :] == targets[:, None, None]) & (
        row_slot[None, None, :] == wanted_slot[None, :, None]
    )
    block_ids = jnp.arange(BLOCKS, dtype=jnp.int32)
    picked_index = jnp.sum(matches.astype(jnp.int32) * block_ids[None, None, :], axis=2).reshape(-1)
    present = jnp.any(matches, axis=2).reshape(-1)
    return (picked_index, present)


def route_blocks(blocks, streams, destination, group_id, dp_index):
    dp_count = lax.axis_size("dp")
    dest_count = 2 * dp_count
    capacity = BLOCKS // 4
    flat_dest, dest_rank, dest_slot = route_tables(destination, dest_count)
    serial = jnp.arange(dest_count, dtype=jnp.int32)
    outgoing = []
    for source_blocks, stream in zip(blocks, streams):
        picked_index, present = send_index(
            flat_dest, dest_slot, stream * dp_count + dp_index, serial, capacity
        )
        present = present & (group_id == stream)
        picked = jnp.take(source_blocks, picked_index, axis=0).reshape(dest_count * capacity, -1)
        outgoing.append(jnp.where(present[:, None], picked, jnp.zeros_like(picked)))
    packed = jnp.concatenate(outgoing, axis=1)
    spare_rows = jnp.zeros_like(packed)
    moved_rows = lax.all_to_all(
        jnp.concatenate([spare_rows, packed], axis=0),
        ("group", "dp"),
        split_axis=0,
        concat_axis=0,
        tiled=True,
    )
    arrived = moved_rows[: dest_count * capacity]
    my_index = (group_id - 2) * dp_count + dp_index
    on_backbone = group_id >= 2
    block_count = flat_dest.shape[0]
    source_slot = jnp.arange(block_count, dtype=jnp.int32) // BLOCKS * capacity + dest_slot
    results = []
    offset = 0
    for source_blocks, stream in zip(blocks, streams):
        slot_width = source_blocks[0].size
        columns = arrived[:, offset : offset + slot_width]
        offset = offset + slot_width
        wanted = stream * (BLOCKS // 2) + jnp.arange(BLOCKS // 2, dtype=jnp.int32)
        matches = (flat_dest[None, :] == my_index) & (dest_rank[None, :] == wanted[:, None])
        picked_index = jnp.sum(matches.astype(jnp.int32) * source_slot[None, :], axis=1)
        taken_rows = jnp.take(columns, picked_index, axis=0)
        taken_rows = jnp.where(on_backbone, taken_rows, jnp.zeros_like(taken_rows))
        results.append(taken_rows.reshape((wanted.shape[0],) + source_blocks.shape[1:]))
    return results


def project(audio_rows, image_rows, audio_active, image_active, audio_proj, image_proj):

    def folder(row_block, active, running, shard_part):
        return lax.cond(
            active,
            lambda inner: jnp.dot(row_block, shard_part, preferred_element_type=jnp.float32),
            lambda inner: inner,
            running,
        )

    audio_start = jnp.zeros((audio_rows.shape[0], audio_proj.shape[1]), jnp.float32)
    image_start = jnp.zeros((image_rows.shape[0], image_proj.shape[1]), jnp.float32)
    audio_out = folder(
        audio_rows, audio_active, audio_start, lax.all_gather(audio_proj, "dp", axis=0, tiled=True)
    )
    image_out = folder(
        image_rows, image_active, image_start, lax.all_gather(image_proj, "dp", axis=0, tiled=True)
    )
    return (audio_out, image_out)


def shards_general(
    audio_states,
    image_states,
    audio_gain,
    image_gain,
    audio_proj,
    image_proj,
    block_rows,
    destination,
    input_gain,
    kv_weight,
):
    group_id = lax.axis_index("group")
    dp_index = lax.axis_index("dp")
    mp_index = lax.axis_index("mp")
    mp_count = lax.axis_size("mp")
    share = BLOCK // mp_count
    row_ids = mp_index * share + jnp.arange(share, dtype=jnp.int32)

    def encode(states, gain_vec, stream):
        limits = lax.dynamic_index_in_dim(block_rows[stream], dp_index, 0, keepdims=False)
        keep_rows = (row_ids[None, :] < limits[:, None]).astype(jnp.float32)
        normed = layer_norm(states[0], gain_vec).reshape(BLOCKS, share, -1)
        return (normed * keep_rows[:, :, None]).astype(jnp.bfloat16)

    audio_normed = encode(audio_states, audio_gain, 0)
    image_normed = encode(image_states, image_gain, 1)
    on_backbone = group_id >= 2
    audio_part, image_part = route_blocks(
        (audio_normed, image_normed), (0, 1), destination, group_id, dp_index
    )
    audio_full, image_full = (
        lax.all_gather(audio_part, "mp", axis=1, tiled=True),
        lax.all_gather(image_part, "mp", axis=1, tiled=True),
    )
    audio_out, image_out = project(
        audio_full.reshape(-1, audio_full.shape[2]),
        image_full.reshape(-1, image_full.shape[2]),
        on_backbone,
        on_backbone,
        audio_proj,
        image_proj,
    )
    arrived = (
        jnp.concatenate([audio_out, image_out], axis=0)
        .astype(jnp.bfloat16)
        .reshape(BLOCKS, BLOCK, -1)
    )
    token_rows = arrived.reshape(BLOCKS * BLOCK, -1)
    tokens = token_rows.astype(jnp.float32)
    squares = lax.psum(jnp.sum(tokens * tokens, axis=1), "mp")
    scaled = (tokens * input_gain).astype(jnp.bfloat16)
    partial_value = jnp.dot(scaled, kv_weight, preferred_element_type=jnp.float32)
    summed = lax.psum_scatter(partial_value, "mp", scatter_dimension=1, tiled=True)
    full_width = tokens.shape[1] * mp_count
    result = summed * lax.rsqrt(squares / full_width + EPS_ROOT)[:, None]
    return (result.astype(jnp.bfloat16)[None], token_rows[None])


MIB = 1 << 20
LANES = 128


class Place:
    def __getitem__(self, axis):
        return lax.axis_index(("group", "dp", "mp")[axis])


def vmem():
    return pl.BlockSpec(memory_space=pltpu.VMEM)


def hbm():
    return pl.BlockSpec(memory_space=pltpu.HBM)


def in_hbm(arrays):
    return [pltpu.with_memory_space_constraint(x, pltpu.HBM) for x in arrays]


def limits_of(mib, flops=0):
    return dict(
        compiler_params=pltpu.CompilerParams(vmem_limit_bytes=mib * MIB),
        cost_estimate=pl.CostEstimate(flops=flops, transcendentals=0, bytes_accessed=0),
    )


def encode_kernel(dp_count, dest, limits, *refs):
    meta = Place()
    group, dp, mp = meta[0], meta[1], meta[2]
    targets = 2 * dp_count
    inputs, messages, scratch = refs[:4], refs[4 : 4 + 2 * targets], refs[4 + 2 * targets :]
    routes, lives, *places, sems = scratch
    for stream in range(2):
        states, gain = places[2 * stream : 2 * stream + 2]
        share = states.shape[1] // BLOCKS
        half = states.shape[2] // dp_count
        outs = messages[stream * targets : (stream + 1) * targets]

        @pl.when(group == stream)
        def _():
            copies = [
                pltpu.make_async_copy(source, place, sems.at[i])
                for i, (source, place) in enumerate(
                    (
                        (dest, routes),
                        (limits, lives),
                        (inputs[2 * stream + 1], gain),
                    )
                )
            ]
            for b in range(BLOCKS):
                part = (0, pl.ds(b * share, share))
                copies.append(
                    pltpu.make_async_copy(
                        inputs[2 * stream].at[part], states.at[part], sems.at[len(copies)]
                    )
                )
            for copy in copies:
                copy.start()
            for copy in copies:
                copy.wait()
            scale = gain[...].reshape(1, -1)
            for target in range(targets):
                block = jnp.int32(0)
                for b in range(BLOCKS):
                    block = jnp.where(routes[stream, dp, b] == target, b, block)
                limit = lives[stream, dp, block]
                start = pl.multiple_of(block * share, share)
                values = states[0, pl.ds(start, share), :].astype(jnp.float32)
                center = values - jnp.mean(values, axis=-1, keepdims=True)
                spread = jnp.mean(center * center, axis=-1, keepdims=True)
                normed = center * lax.rsqrt(spread + EPS_LAYER) * scale
                row = mp * share + lax.broadcasted_iota(jnp.int32, normed.shape, 0)
                normed = jnp.where(row < limit, normed, 0.0).astype(jnp.bfloat16)
                c, home = target // dp_count, target % dp_count
                for k in range(dp_count):
                    place = 0 if home == k else 1
                    outs[c * dp_count + k][place * share : (place + 1) * share, :] = normed[
                        :, k * half : (k + 1) * half
                    ]


def encode(dp_count, dest, limits, streams):
    arguments, shapes = [], []
    scratch = [pltpu.SMEM(dest.shape, jnp.int32), pltpu.SMEM(limits.shape, jnp.int32)]
    for states, gain, _ in streams:
        arguments += [states, gain]
        scratch += [pltpu.VMEM(states.shape, states.dtype), pltpu.VMEM(gain.shape, gain.dtype)]
        _, rows, width = states.shape
        shape = jax.ShapeDtypeStruct((2 * rows // BLOCKS, width // dp_count), jnp.bfloat16)
        shapes += [shape] * (2 * dp_count)
    return pl.pallas_call(
        functools.partial(encode_kernel, dp_count),
        out_shape=shapes,
        in_specs=[hbm()] * (2 + len(arguments)),
        out_specs=[vmem()] * len(shapes),
        scratch_shapes=scratch + [pltpu.SemaphoreType.DMA((3 + BLOCKS,))],
        name="encode",
        **limits_of(8, 1 << 28),
    )(*in_hbm([dest, limits, *arguments]))


def fetch_kernel(cuts, *refs):
    count = len(cuts)
    sources, places, sems = refs[:count], refs[count : 2 * count], refs[2 * count]
    copies = []
    for source, place, pieces in zip(sources, places, cuts):
        depth = source.shape[0] // pieces
        for i in range(pieces):
            part = pl.ds(i * depth, depth)
            copies.append(
                pltpu.make_async_copy(source.at[part], place.at[part], sems.at[len(copies)])
            )
    for copy in copies:
        copy.start()
    for copy in copies:
        copy.wait()


def fetch(weights, cuts):
    return pl.pallas_call(
        functools.partial(fetch_kernel, cuts),
        out_shape=[pltpu.VMEM(x.shape, x.dtype) for x in weights],
        in_specs=[hbm()] * len(weights),
        out_specs=[vmem()] * len(weights),
        scratch_shapes=[pltpu.SemaphoreType.DMA((sum(cuts),))],
        name="fetch",
        **limits_of(12, 1 << 28),
    )(*in_hbm(weights))


def piece_source(mp, shift, mp_count):
    if mp_count == 4:
        return mp ^ shift
    return lax.rem(mp + (mp_count - shift), mp_count)


def project_half_kernel(mp_count, tile, half, *refs):
    meta = Place()
    pieces, weight, result, rows = refs[:mp_count], *refs[mp_count:]
    share = pieces[0].shape[0] // 2
    for shift in range(mp_count):
        start = pl.multiple_of(piece_source(meta[2], shift, mp_count) * share, share)
        rows[pl.ds(start, share), :] = pieces[shift][half * share : (half + 1) * share, :]
    for first in range(0, weight.shape[1], tile):
        out = jnp.dot(
            rows[...], weight[:, first : first + tile], preferred_element_type=jnp.float32
        )
        result[:, first : first + tile] = out.astype(result.dtype)


def project_half(mp_count, pieces, weight, tile, half):
    depth, width = weight.shape
    rows = pieces[0].shape[0] * mp_count // 2
    kind = jnp.bfloat16 if half else jnp.float32
    return pl.pallas_call(
        functools.partial(project_half_kernel, mp_count, tile, half),
        out_shape=jax.ShapeDtypeStruct((rows, width), kind),
        in_specs=[vmem()] * (mp_count + 1),
        out_specs=vmem(),
        scratch_shapes=[pltpu.VMEM((rows, depth), jnp.bfloat16)],
        name="project",
        **limits_of(12, 2 * rows * depth * width),
    )(*pieces, weight)


def project_kernel(mp_count, tile, *refs):
    meta = Place()
    pieces, weight, keep, send, rows = refs[:mp_count], *refs[mp_count:]
    share = pieces[0].shape[0] // 2
    block = share * mp_count
    for shift in range(mp_count):
        source = piece_source(meta[2], shift, mp_count)
        start = pl.multiple_of(source * share, share)
        rows[pl.ds(start, share), :] = pieces[shift][:share, :]
        rows[pl.ds(block + start, share), :] = pieces[shift][share:, :]
    for first in range(0, weight.shape[1], tile):
        out = jnp.dot(
            rows[...], weight[:, first : first + tile], preferred_element_type=jnp.float32
        )
        keep[:, first : first + tile] = out[:block]
        send[:, first : first + tile] = out[block:].astype(jnp.bfloat16)


def project_rows(mp_count, pieces, weight, tile):
    depth, width = weight.shape
    rows = pieces[0].shape[0] * mp_count
    return pl.pallas_call(
        functools.partial(project_kernel, mp_count, tile),
        out_shape=[
            jax.ShapeDtypeStruct((rows // 2, width), jnp.float32),
            jax.ShapeDtypeStruct((rows // 2, width), jnp.bfloat16),
        ],
        in_specs=[vmem()] * (mp_count + 1),
        out_specs=[vmem()] * 2,
        scratch_shapes=[pltpu.VMEM((rows, depth), jnp.bfloat16)],
        name="project",
        **limits_of(12, 2 * rows * depth * width),
    )(*pieces, weight)


def heads_kernel(mp_count, keep, other, gain, weight, tokens, own, *rest):
    meta = Place()
    sends, scaled = rest[:-1], rest[-1]
    rows, tile = tokens.shape[0], weight.shape[1] // mp_count
    rounded = (keep[...] + other[...].astype(jnp.float32)).astype(jnp.bfloat16)
    tokens[...] = rounded
    values = rounded.astype(jnp.float32)
    scaled[...] = (values * gain[...].reshape(1, -1)).astype(jnp.bfloat16)
    total = jnp.sum(values * values, axis=1, keepdims=True)
    turned = jnp.transpose(jnp.broadcast_to(total, (rows, LANES)))[:8]
    high = turned.astype(jnp.bfloat16).astype(jnp.float32)
    line = lax.broadcasted_iota(jnp.int32, turned.shape, 0)
    packed = jnp.where(line == 0, high, jnp.where(line == 1, turned - high, 0.0))
    for shift in list(range(1, mp_count)) + [0]:
        chunk = lax.rem(meta[2] + shift, mp_count)
        columns = pl.ds(pl.multiple_of(chunk * tile, tile), tile)
        out = jnp.dot(scaled[...], weight[:, columns], preferred_element_type=jnp.float32)
        place = sends[shift - 1] if shift else own
        for q in range(tile // LANES):
            part = out[:, q * LANES : (q + 1) * LANES]
            place[q * rows : (q + 1) * rows, :] = part.astype(place.dtype)
        place[rows * tile // LANES :, :] = packed.astype(place.dtype)


def heads(mp_count, keep, other, gain, weight):
    rows, width = keep.shape
    tile = weight.shape[1] // mp_count
    return pl.pallas_call(
        functools.partial(heads_kernel, mp_count),
        in_specs=[vmem()] * 4,
        out_specs=[vmem()] * (1 + mp_count),
        scratch_shapes=[pltpu.VMEM((rows, width), jnp.bfloat16)],
        out_shape=[
            jax.ShapeDtypeStruct((rows, width), jnp.bfloat16),
            jax.ShapeDtypeStruct((rows * tile // LANES + 8, LANES), jnp.float32),
        ]
        + [jax.ShapeDtypeStruct((rows * tile // LANES + 8, LANES), jnp.bfloat16)] * (mp_count - 1),
        name="heads",
        **limits_of(14, 2 * rows * width * weight.shape[1]),
    )(keep, other, gain, weight)


def finish_kernel(full_width, own, *refs):
    parts, result = refs[:-1], refs[-1]
    rows = result.shape[0]
    total = own[...]
    for part in parts:
        total = total + part[...].astype(jnp.float32)
    last = total.shape[0] - 8
    square = total[last : last + 1] + total[last + 1 : last + 2]
    scale = lax.rsqrt(square / full_width + EPS_ROOT)
    column = jnp.transpose(jnp.broadcast_to(scale, (LANES, rows)))[:, :1]
    for q in range(last // rows):
        part = total[q * rows : (q + 1) * rows] * column
        result[:, q * LANES : (q + 1) * LANES] = part.astype(jnp.bfloat16)


def finish(full_width, rows, own, parts):
    tile = (own.shape[0] - 8) // rows * LANES
    return pl.pallas_call(
        functools.partial(finish_kernel, full_width),
        out_shape=jax.ShapeDtypeStruct((rows, tile), jnp.bfloat16),
        in_specs=[vmem()] * (1 + len(parts)),
        out_specs=vmem(),
        name="finish",
        **limits_of(4, 1 << 26),
    )(own, *parts)


def place_early_kernel(kept0, kept1, moved0, out, zeros, sems):
    meta = Place()
    rows = kept0.shape[0]
    at = lambda place: out.at[pl.ds(place * rows, rows)]

    @pl.when(meta[0] >= 2)
    def _():
        copies = [
            pltpu.make_async_copy(source, at(place), sems.at[place])
            for source, place in ((moved0, 0), (kept0, 1), (kept1, 3))
        ]
        for copy in copies:
            copy.start()
        for copy in copies:
            copy.wait()

    @pl.when(meta[0] < 2)
    def _():
        zeros[...] = jnp.zeros_like(zeros)
        copies = [
            pltpu.make_async_copy(zeros, at(place), sems.at[place]) for place in range(BLOCKS)
        ]
        for copy in copies:
            copy.start()
        for copy in copies:
            copy.wait()


def place_early(kept, moved):
    rows, width = moved.shape
    return pl.pallas_call(
        place_early_kernel,
        out_shape=pltpu.HBM((BLOCKS * rows, width), moved.dtype),
        in_specs=[pl.BlockSpec(memory_space=pl.ANY)] * 3,
        out_specs=hbm(),
        scratch_shapes=[pltpu.VMEM((rows, width), moved.dtype), pltpu.SemaphoreType.DMA((BLOCKS,))],
        name="place",
        **limits_of(4, 1 << 26),
    )(*kept, moved)


def place_late_kernel(moved1, before, out, sem):
    meta = Place()
    rows = moved1.shape[0]

    @pl.when(meta[0] >= 2)
    def _():
        copy = pltpu.make_async_copy(moved1, out.at[pl.ds(2 * rows, rows)], sem)
        copy.start()
        copy.wait()


def place_late(moved, rows_out):
    return pl.pallas_call(
        place_late_kernel,
        out_shape=pltpu.HBM(rows_out.shape, rows_out.dtype),
        in_specs=[pl.BlockSpec(memory_space=pl.ANY), hbm()],
        out_specs=hbm(),
        scratch_shapes=[pltpu.SemaphoreType.DMA],
        input_output_aliases={1: 0},
        name="place",
        **limits_of(4, 1 << 26),
    )(moved, rows_out)


def shards_direct(
    audio_states,
    image_states,
    audio_gain,
    image_gain,
    audio_proj,
    image_proj,
    block_rows,
    destination,
    input_gain,
    kv_weight,
):
    group = lax.axis_index("group")
    dp = lax.axis_index("dp")
    dp_count = lax.axis_size("dp")
    mp_count = lax.axis_size("mp")
    rings = [[(i, (i + shift) % mp_count) for i in range(mp_count)] for shift in range(mp_count)]
    spreads = rings
    if mp_count == 4:
        spreads = [[(i, i ^ step) for i in range(mp_count)] for step in (0, 1, 2, 1)]
    swap = [(i, (i + 1) % dp_count) for i in range(dp_count)]
    up = [(0, 2), (1, 3)]
    full_width = input_gain.shape[0] * mp_count
    targets = 2 * dp_count
    streams = (
        (audio_states, audio_gain, audio_proj),
        (image_states, image_gain, image_proj),
    )

    messages = encode(dp_count, destination, block_rows, streams)
    mine = lax.rem(group, 2) * dp_count + dp
    gathered = []
    for stream in range(2):
        piece = None
        for index in range(targets):
            c, k = index // dp_count, index % dp_count
            pairs = [(stream * dp_count + d, (2 * d + c) * dp_count + k) for d in range(dp_count)]
            moved = lax.ppermute(messages[stream * targets + index], ("group", "dp"), pairs)
            piece = moved if piece is None else jnp.where(mine == index, moved, piece)
        pieces = [piece]
        for shift in range(1, mp_count):
            sent = pieces[2] if mp_count == 4 and shift == 3 else piece
            pieces.append(lax.ppermute(sent, "mp", spreads[shift]))
        gathered.append(pieces)
    partial, others = [], []
    for stream, (_, _, proj) in enumerate(streams):
        (proj,) = fetch([proj], (4,))
        if stream == 0:
            keep, send = project_rows(mp_count, gathered[stream], proj, 512)
        else:
            send = project_half(mp_count, gathered[stream], proj, 512, 1)
            keep = project_half(mp_count, gathered[stream], proj, 512, 0)
        partial.append((keep, send))
        others.append(lax.ppermute(send, "dp", swap))
    (heads_weight,) = fetch([kv_weight], (8,))
    kept, moved, head_parts = [], [], []
    for stream in range(2):
        tokens, own, *sends = heads(
            mp_count, partial[stream][0], others[stream], input_gain, heads_weight
        )
        sums = []
        for shift, part in enumerate(sends, 1):
            sums.append(lax.ppermute(part, "mp", rings[shift]))
        kept.append(tokens)
        moved.append(lax.ppermute(tokens, "group", up))
        values = finish(full_width, tokens.shape[0], own, sums)
        head_parts += [lax.ppermute(values, "group", up), values]
    rows_out = place_early(kept, moved[0])
    rows_out = place_late(moved[1], rows_out)
    heads_out = place_early([head_parts[1], head_parts[3]], head_parts[0])
    heads_out = place_late(head_parts[2], heads_out)
    return (heads_out[None], rows_out[None])


def solution(mesh):
    if 2 * mesh.shape["dp"] != BLOCKS:
        return mapped(shards_general, mesh)
    layer = lambda *inputs: shards_direct(*inputs)
    return mapped(layer, mesh)


def mapped(shards, mesh):
    in_specs = (
        P("group", ("dp", "mp"), None),
        P("group", ("dp", "mp"), None),
        P(),
        P(),
        P("dp", "mp"),
        P("dp", "mp"),
        P(),
        P(),
        P("mp"),
        P("mp", None),
    )
    out_specs = (P("group", "dp", "mp"), P("group", "dp", "mp"))
    return jax.shard_map(shards, mesh=mesh, in_specs=in_specs, out_specs=out_specs, check_vma=False)
```
